128 devices in a mesh: data: 1, node: 2 (over core), expert: 64 (over z, y, x).
Axes of the slice: x: 4, y: 4, z: 4, core: 2. Of those that a mesh axis runs over, the one named last changes fastest.
Arguments:
- tokens: bfloat16 [32768, 2048], P(('data', 'node', 'expert'))
- expert_ids: int32 [32768, 8], P(('data', 'node', 'expert'))
- gate_weights: float32 [32768, 8], P(('data', 'node', 'expert'))
- slot_ids: int32 [32768, 8], P(('data', 'node', 'expert'))
- w_gate: bfloat16 [128, 2048, 768], P(('node', 'expert'))
- w_up: bfloat16 [128, 2048, 768], P(('node', 'expert'))
- w_down: bfloat16 [128, 768, 2048], P(('node', 'expert'))
Outputs:
- output: bfloat16 [32768, 2048], P(('data', 'node', 'expert'))
All inputs are finite; a program needn't handle non-finite values.
Results may differ from the reference program's by a relative error of at most 0.00153.
Values are sent between devices in bfloat16 or wider.
A program may use at most 1 GiB of HBM per device.

```python
import jax
import jax.numpy as jnp
from jax import lax

EXPERTS = 128
D = 2048
FF = 768
TOP = 8
TOKENS_DEV = 256
GROUP = 128
CAP = 32

TOKENS = GROUP * TOKENS_DEV


def device_slots(flat_ids):
    choice_count = flat_ids.shape[0]
    sort_order = jnp.argsort(flat_ids, stable=True)
    sorted_ids = flat_ids[sort_order]
    counts = jnp.zeros((EXPERTS,), jnp.int32).at[flat_ids].add(1)
    starts = jnp.cumsum(counts) - counts
    rank_sorted = jnp.arange(choice_count, dtype=jnp.int32) - starts[sorted_ids]
    rank_all = jnp.zeros((choice_count,), jnp.int32).at[sort_order].set(rank_sorted)
    return jnp.where(rank_all < CAP, rank_all, -1)


def draw_routing(key):
    sub_keys = jax.random.split(key, 5)
    hot_first = jax.random.randint(sub_keys[0], (), 0, EXPERTS)
    pick_hot = jax.random.randint(sub_keys[1], (TOKENS,), 0, 4)
    hot_base = jax.random.randint(sub_keys[2], (TOKENS,), 0, max(EXPERTS // 4, 1))
    any_base = jax.random.randint(sub_keys[3], (TOKENS,), 0, EXPERTS)
    base_ids = jnp.where(pick_hot == 0, hot_base, any_base)
    local_row = jnp.arange(TOKENS, dtype=jnp.int32) % TOKENS_DEV
    base_ids = jnp.where(local_row < CAP, 0, base_ids)
    step_max = (EXPERTS - 1) // max(TOP - 1, 1)
    step_sizes = jax.random.randint(sub_keys[4], (TOKENS, TOP), 1, step_max + 1)
    step_sizes = step_sizes.at[:, 0].set(0)
    offsets = jnp.cumsum(step_sizes, axis=1)
    expert_ids = ((base_ids[:, None] + hot_first + offsets) % EXPERTS).astype(jnp.int32)
    slot_ids = jax.vmap(device_slots)(expert_ids.reshape(GROUP, TOKENS_DEV * TOP))
    return expert_ids, slot_ids.reshape(TOKENS, TOP).astype(jnp.int32)


def setup_inputs(seed: int = 0, part: int = 0) -> dict:
    part_key = jax.random.fold_in(jax.random.key(seed), part)
    key_tokens, key_route, key_gates = jax.random.split(part_key, 3)
    key_gate_w, key_up_w, key_down_w = jax.random.split(jax.random.key(seed + 1), 3)
    tokens = jax.random.normal(key_tokens, (TOKENS, D), jnp.float32).astype(jnp.bfloat16)
    expert_ids, slot_ids = draw_routing(key_route)
    gate_weights = (0.5 + jax.random.uniform(key_gates, (TOKENS, TOP), jnp.float32)) * TOP ** -0.5
    w_gate = (jax.random.normal(key_gate_w, (EXPERTS, D, FF), jnp.float32) * D ** -0.5).astype(jnp.bfloat16)
    w_up = (jax.random.normal(key_up_w, (EXPERTS, D, FF), jnp.float32) * D ** -0.5).astype(jnp.bfloat16)
    w_down = (jax.random.normal(key_down_w, (EXPERTS, FF, D), jnp.float32) * FF ** -0.5).astype(jnp.bfloat16)
    return {"tokens": tokens, "expert_ids": expert_ids, "gate_weights": gate_weights, "slot_ids": slot_ids, "w_gate": w_gate, "w_up": w_up, "w_down": w_down}


def expert_block(expert_rows, gate_mat, up_mat, down_mat):
    proj_gate = jnp.dot(expert_rows, gate_mat, preferred_element_type=jnp.float32)
    proj_up = jnp.dot(expert_rows, up_mat, preferred_element_type=jnp.float32)
    hidden = (jax.nn.silu(proj_gate) * proj_up).astype(jnp.bfloat16)
    return jnp.dot(hidden, down_mat, preferred_element_type=jnp.float32).astype(jnp.bfloat16)


def reference(tokens, expert_ids, gate_weights, slot_ids, w_gate, w_up, w_down):
    buffer_rows = GROUP * CAP
    source_dev = (jnp.arange(TOKENS, dtype=jnp.int32) // TOKENS_DEV)[:, None]
    kept = slot_ids >= 0
    flat_pos = jnp.where(kept, expert_ids * buffer_rows + source_dev * CAP + slot_ids, EXPERTS * buffer_rows).reshape(-1)
    tok_index = jnp.broadcast_to(jnp.arange(TOKENS, dtype=jnp.int32)[:, None], (TOKENS, TOP)).reshape(-1)
    src_table = jnp.full((EXPERTS * buffer_rows,), TOKENS, jnp.int32).at[flat_pos].set(tok_index, mode="drop")
    gate_table = jnp.zeros((EXPERTS * buffer_rows,), jnp.float32).at[flat_pos].set(gate_weights.reshape(-1), mode="drop")

    def one_expert(out_sum, operands):
        src_rows, row_gates, gate_mat, up_mat, down_mat = operands
        expert_rows = jnp.take(tokens, src_rows, axis=0, mode="fill", fill_value=0)
        expert_out = expert_block(expert_rows, gate_mat, up_mat, down_mat)
        out_sum = out_sum.at[src_rows].add(row_gates[:, None] * expert_out.astype(jnp.float32), mode="drop")
        return out_sum, None

    out_sum, _ = lax.scan(one_expert, jnp.zeros((TOKENS, D), jnp.float32), (src_table.reshape(EXPERTS, buffer_rows), gate_table.reshape(EXPERTS, buffer_rows), w_gate, w_up, w_down))
    return out_sum.astype(jnp.bfloat16)
```

```python
import jax
import jax.numpy as jnp
from jax import lax
from jax.experimental import pallas as pl
from jax.experimental.pallas import tpu as pltpu
from jax.sharding import PartitionSpec as P

MESH = pl.DeviceIdType.MESH
CAP_FACTOR = 2
RING = 4
DELTAS = (1, 3, 2)
COLS = ((0, 768), (768, 640), (1408, 640))
STRIDES = ((16, 4, 1), (4, 1, 16))


def capacity(rows, top_k, experts):
    return ((CAP_FACTOR * rows * top_k + 8 * experts - 1) // (8 * experts)) * 8


def place():
    core, e = lax.axis_index("node"), lax.axis_index("expert")
    z, y, x = e // 16, (e // 4) % 4, e % 4
    return core, e, ((z, y, x), (y, x, z))


def own_view(core, views):
    v = tuple(a + core * (b - a) for a, b in zip(*views))
    s = tuple(a + core * (b - a) for a, b in zip(*STRIDES))
    return v, s


def step(e, pos, stride, delta):
    return e + (lax.rem(pos + delta, RING) - pos) * stride


def cols(k):
    return pl.ds(*COLS[k])


def dims(k):
    return k % 3, (k + 1) % 3, (k + 2) % 3


def plane_at(k, d0, d1):
    return (d1, d0) if k == 2 else (d0, d1)


def cube_at(k, p):
    full = [slice(None)] * 3
    full[dims(k)[2]] = p
    return tuple(full)


def remote(src, dst, send, recv, core, e):
    return pltpu.make_async_remote_copy(src_ref=src, dst_ref=dst, send_sem=send, recv_sem=recv, device_id=(0, core, e), device_id_type=MESH)


def greet(targets):
    barrier = pltpu.get_barrier_semaphore()
    for core, e in targets:
        pl.semaphore_signal(barrier, inc=1, device_id=(0, core, e), device_id_type=MESH)
    pl.semaphore_wait(barrier, len(targets))


def ring_peers(core_list, e, views):
    out = []
    for core in core_list:
        for v, s in zip(views[0], STRIDES[0]):
            for delta in DELTAS:
                out.append((core, step(e, v, s, delta)))
    return out


def spread_kernel(tok, meta, t2, mt, loc, s1s, s1r, m1s, m1r, s2s, s2r, m2s, m2r, s3s, s3r):
    core, e, views = place()
    v, st = own_view(core, views)
    greet(ring_peers((core,), e, views))
    half = tok.shape[0] // 2
    sends, locals_ = [], []

    def go(copy):
        copy.start()
        sends.append(copy)

    for k in range(3):
        i0, i1, _ = dims(k)
        here = plane_at(k, v[i0], v[i1])
        for delta in DELTAS:
            peer = step(e, v[i0], st[i0], delta)
            go(remote(tok.at[:, cols(k)], t2.at[(*here, slice(None), cols(k))], s1s.at[k, delta - 1], s1r.at[k, delta - 1], core, peer))
            go(remote(meta, mt.at[(k, *here)], m1s.at[k, delta - 1], m1r.at[k, delta - 1], core, peer))
    for k in range(3):
        i0, i1, _ = dims(k)
        here = plane_at(k, v[i0], v[i1])
        own = pltpu.make_async_copy(tok.at[:, cols(k)], t2.at[(*here, slice(None), cols(k))], loc.at[0, k])
        own.start()
        locals_.append(own)
        own = pltpu.make_async_copy(meta, mt.at[(k, *here)], loc.at[1, k])
        own.start()
        locals_.append(own)

    def second(k, j):
        i0, i1, _ = dims(k)
        at = plane_at(k, lax.rem(v[i0] + j, RING), v[i1])
        block = t2.at[(*at, slice(None), cols(k))]
        for way, delta in enumerate((1, 3)):
            src = tok.at[:, cols(k)] if j == 0 else block
            go(remote(src, block, s2s.at[k, j, way], s2r.at[k, j, way], core, step(e, v[i1], st[i1], delta)))
        for delta in DELTAS:
            src = meta if j == 0 else mt.at[(k, *at)]
            go(remote(src, mt.at[(k, *at)], m2s.at[k, j, delta - 1], m2r.at[k, j, delta - 1], core, step(e, v[i1], st[i1], delta)))

    for k in range(3):
        second(k, 0)
    for j in DELTAS:
        for k in range(3):
            i0, i1, _ = dims(k)
            at = plane_at(k, lax.rem(v[i0] + j, RING), v[i1])
            block = t2.at[(*at, slice(None), cols(k))]
            remote(block, block, s1s.at[k, 3 - j], s1r.at[k, 3 - j], core, e).wait_recv()
            remote(mt.at[(k, *at)], mt.at[(k, *at)], m1s.at[k, 3 - j], m1r.at[k, 3 - j], core, e).wait_recv()
            second(k, j)
    for j in (0, *DELTAS):
        for k in range(3):
            i0, i1, _ = dims(k)
            for way, delta in enumerate((1, 3)):
                at = plane_at(k, lax.rem(v[i0] + j, RING), lax.rem(v[i1] + 4 - delta, RING))
                block = t2.at[(*at, slice(None), cols(k))]
                remote(block, block, s2s.at[k, j, way], s2r.at[k, j, way], core, e).wait_recv()
                part = t2.at[(*at, pl.ds(half * way, half), cols(k))]
                go(remote(part, part, s3s.at[k, j, way], s3r.at[k, j, way], core, step(e, v[i1], st[i1], delta)))
    for j in (0, *DELTAS):
        for k in range(3):
            i0, i1, _ = dims(k)
            for delta in DELTAS:
                at = plane_at(k, lax.rem(v[i0] + j, RING), lax.rem(v[i1] + 4 - delta, RING))
                remote(mt.at[(k, *at)], mt.at[(k, *at)], m2s.at[k, j, delta - 1], m2r.at[k, j, delta - 1], core, e).wait_recv()
            at = plane_at(k, lax.rem(v[i0] + j, RING), lax.rem(v[i1] + 2, RING))
            for way in range(2):
                part = t2.at[(*at, pl.ds(half * way, half), cols(k))]
                remote(part, part, s3s.at[k, j, way], s3r.at[k, j, way], core, e).wait_recv()
    for copy in sends:
        copy.wait_send()
    for copy in locals_:
        copy.wait()


def pick_kernel(slots, t2, mt, out):
    core, e, views = place()
    v, st = own_view(core, views)
    rows = RING * 2 * slots
    r = lax.broadcasted_iota(jnp.int32, (rows, 1), 0)
    p2, half, s = r // (2 * slots), (r // slots) % 2, r % slots
    for k in range(3):
        i0, i1, i2 = dims(k)
        key = ((half * 64 + v[i0] * st[i0] + v[i1] * st[i1] + p2 * st[i2]) * slots + s).astype(jnp.float32)
        hot = jnp.zeros((rows, t2.shape[2]), jnp.float32)
        for j in range(8):
            hot = jnp.where(key == mt[k, 0, 0, j:j + 1, :], 1.0, hot)
        got = jnp.dot(hot.astype(jnp.bfloat16), t2[0, 0, :, cols(k)], preferred_element_type=jnp.float32)
        out[:, :, 0, 0, :, cols(k)] = got.astype(jnp.bfloat16).reshape(RING, 2, slots, COLS[k][1])


def out_kernel(s_ref, r_ref, bounce, loc, ss, rs):
    core, e, views = place()
    v, st = own_view(core, views)
    greet(ring_peers((0, 1), e, views) + [(1 - core, e)])
    sends = []
    for delta in (1, 3, 2):
        for k in range(3):
            i2 = dims(k)[2]
            p = lax.rem(v[i2] + delta, RING)
            for to in range(2):
                copy = remote(s_ref.at[p, to, :, :, :, cols(k)], r_ref.at[(core, *cube_at(k, v[i2]), slice(None), cols(k))], ss.at[k, delta, to], rs.at[k, delta, core], to, step(e, v[i2], st[i2], delta))
                copy.start()
                sends.append(copy)
    ins, outs = [], []
    for k in range(3):
        i2 = dims(k)[2]
        target = r_ref.at[(core, *cube_at(k, v[i2]), slice(None), cols(k))]
        copy = remote(s_ref.at[v[i2], 1 - core, :, :, :, cols(k)], target, ss.at[k, 0, 0], rs.at[k, 0, 0], 1 - core, e)
        copy.start()
        sends.append(copy)
        room = bounce.at[:, :, :, cols(k)]
        into = pltpu.make_async_copy(s_ref.at[v[i2], core, :, :, :, cols(k)], room, loc.at[0, k])
        into.start()
        ins.append(into)
        outs.append(pltpu.make_async_copy(room, target, loc.at[1, k]))
    for into, out in zip(ins, outs):
        into.wait()
        out.start()
    for out in outs:
        out.wait()
    other = own_view(1 - core, views)[0]
    for k in range(3):
        i2 = dims(k)[2]
        target = r_ref.at[(1 - core, *cube_at(k, other[i2]), slice(None), cols(k))]
        remote(target, target, ss.at[k, 0, 0], rs.at[k, 0, 0], core, e).wait_recv()
        for delta in (1, 3, 2):
            for o in range(2):
                target = r_ref.at[(o, *cube_at(k, lax.rem(views[o][i2] + 4 - delta, RING)), slice(None), cols(k))]
                remote(target, target, ss.at[k, delta, 0], rs.at[k, delta, o], core, e).wait_recv()
    for copy in sends:
        copy.wait_send()


def back_kernel(y_ref, z4, z5, bounce, bounce2, loc, s4, r4, s5, r5):
    core, e, views = place()
    v, st = own_view(core, views)
    greet(ring_peers((0, 1), e, views) + [(1 - core, e)])
    sends = []
    for delta in (1, 3, 2):
        for k in range(3):
            i2 = dims(k)[2]
            for o in range(2):
                here = views[o][i2]
                copy = remote(y_ref.at[(o, *cube_at(k, lax.rem(here + delta, RING)), slice(None), cols(k))], z4.at[here, core, :, :, :, cols(k)], s4.at[k, delta, o], r4.at[k, delta, core], o, step(e, here, STRIDES[o][i2], delta))
                copy.start()
                sends.append(copy)
    other = own_view(1 - core, views)[0]
    ins, outs = [], []
    for k in range(3):
        i2 = dims(k)[2]
        copy = remote(y_ref.at[(1 - core, *cube_at(k, other[i2]), slice(None), cols(k))], z4.at[other[i2], core, :, :, :, cols(k)], s4.at[k, 0, 0], r4.at[k, 0, 0], 1 - core, e)
        copy.start()
        sends.append(copy)
        room = bounce.at[:, :, :, cols(k)]
        into = pltpu.make_async_copy(y_ref.at[(core, *cube_at(k, v[i2]), slice(None), cols(k))], room, loc.at[0, k])
        into.start()
        ins.append(into)
        outs.append(pltpu.make_async_copy(room, z4.at[v[i2], core, :, :, :, cols(k)], loc.at[1, k]))
    for into, out in zip(ins, outs):
        into.wait()
        out.start()
    for out in outs:
        out.wait()

    def line(k, q):
        at = (slice(None), slice(None), q, slice(None)) if k == 2 else (slice(None), slice(None), slice(None), q)
        return z4.at[(*at, slice(None), cols(k))]

    ins, outs = [], []
    for k in range(3):
        i1, i2 = dims(k)[1:]
        target = z4.at[v[i2], 1 - core, :, :, :, cols(k)]
        remote(target, target, s4.at[k, 0, 0], r4.at[k, 0, 0], core, e).wait_recv()
        for delta in (1, 3, 2):
            for o in range(2):
                target = z4.at[lax.rem(v[i2] + 4 - delta, RING), o, :, :, :, cols(k)]
                remote(target, target, s4.at[k, delta, 0], r4.at[k, delta, o], core, e).wait_recv()
        for delta in (1, 3, 2):
            copy = remote(line(k, lax.rem(v[i1] + delta, RING)), z5.at[v[i1], :, :, :, :, cols(k)], s5.at[k, delta - 1], r5.at[k, delta - 1], core, step(e, v[i1], st[i1], delta))
            copy.start()
            sends.append(copy)
        room = bounce2.at[:, :, :, :, cols(k)]
        into = pltpu.make_async_copy(line(k, v[i1]), room, loc.at[2, k])
        into.start()
        ins.append(into)
        outs.append(pltpu.make_async_copy(room, z5.at[v[i1], :, :, :, :, cols(k)], loc.at[3, k]))
    for into, out in zip(ins, outs):
        into.wait()
        out.start()
    for out in outs:
        out.wait()
    for k in range(3):
        i1 = dims(k)[1]
        for delta in (1, 3, 2):
            target = z5.at[lax.rem(v[i1] + 4 - delta, RING), :, :, :, :, cols(k)]
            remote(target, target, s5.at[k, delta - 1], r5.at[k, delta - 1], core, e).wait_recv()
    for copy in sends:
        copy.wait_send()


def weigh_kernel(slots, z5, mt, out):
    core, e, views = place()
    v, st = own_view(core, views)
    d0 = pl.program_id(0)
    n = RING * RING * 2 * slots
    r = lax.broadcasted_iota(jnp.int32, (1, n), 1)
    d1, p2, half, s = r // (RING * 2 * slots), (r // (2 * slots)) % RING, (r // slots) % 2, r % slots
    for k in range(3):
        i0, i1, i2 = dims(k)
        a, b = plane_at(k, d0, v[i1])
        m = jnp.transpose(mt[k, a, b])
        key = ((half * 64 + v[i0] * st[i0] + d1 * st[i1] + p2 * st[i2]) * slots + s).astype(jnp.float32)
        w = jnp.zeros((m.shape[0], n), jnp.float32)
        for j in range(8):
            w = jnp.where(m[:, j:j + 1] == key, m[:, 8 + j:9 + j], w)
        hi = w.astype(jnp.bfloat16)
        rest = w - hi.astype(jnp.float32)
        mid = rest.astype(jnp.bfloat16)
        low = (rest - mid.astype(jnp.float32)).astype(jnp.bfloat16)
        y = z5[:, :, :, 0, :, cols(k)].reshape(n, COLS[k][1])
        total = jnp.dot(low, y, preferred_element_type=jnp.float32)
        total += jnp.dot(mid, y, preferred_element_type=jnp.float32)
        total += jnp.dot(hi, y, preferred_element_type=jnp.float32)
        out[0, :, cols(k)] = total


def sum_kernel(p_ref, out, q, loc, ss, rs):
    core, e, views = place()
    v, st = own_view(core, views)
    greet(ring_peers((core,), e, views))
    sends, locals_ = [], []
    for delta in (1, 3, 2):
        for k in range(3):
            i0 = dims(k)[0]
            copy = remote(p_ref.at[lax.rem(v[i0] + delta, RING), :, cols(k)], q.at[delta, :, cols(k)], ss.at[k, delta - 1], rs.at[k, delta - 1], core, step(e, v[i0], st[i0], delta))
            copy.start()
            sends.append(copy)
    for k in range(3):
        copy = pltpu.make_async_copy(p_ref.at[v[dims(k)[0]], :, cols(k)], q.at[0, :, cols(k)], loc.at[k])
        copy.start()
        locals_.append(copy)
    for copy in locals_:
        copy.wait()
    for k in range(3):
        for delta in (1, 3, 2):
            target = q.at[delta, :, cols(k)]
            remote(target, target, ss.at[k, delta - 1], rs.at[k, delta - 1], core, e).wait_recv()

    @pl.loop(0, out.shape[0] // 16)
    def _(i):
        at = pl.ds(pl.multiple_of(i * 16, 16), 16)
        out[at, :] = ((q[0, at, :] + q[1, at, :]) + (q[2, at, :] + q[3, at, :])).astype(jnp.bfloat16)

    for copy in sends:
        copy.wait_send()


def comm_call(body, name, cid, ins, outs, scratch):
    return pl.pallas_call(
        body,
        name=name,
        out_shape=outs,
        in_specs=ins,
        out_specs=[pl.BlockSpec(memory_space=pltpu.HBM)] * len(outs) if isinstance(outs, list) else pl.BlockSpec(memory_space=pltpu.VMEM),
        scratch_shapes=scratch,
        compiler_params=pltpu.CompilerParams(collective_id=cid, has_side_effects=True),
    )


def solution(mesh):
    group_axes = ("node", "expert")
    group_size = mesh.shape["node"] * mesh.shape["expert"]
    tok_spec = P(("data", "node", "expert"), None)
    weight_spec = P(("node", "expert"), None, None)
    hbm = pl.BlockSpec(memory_space=pltpu.HBM)
    vmem = pl.BlockSpec(memory_space=pltpu.VMEM)
    dma = pltpu.SemaphoreType.DMA

    def local_layer(tokens, expert_ids, gate_weights, slot_ids, w_gate, w_up, w_down):
        rows, width = tokens.shape
        top_k = expert_ids.shape[1]
        slots = capacity(rows, top_k, group_size)
        bf = jnp.bfloat16
        pos = jnp.where(slot_ids >= 0, expert_ids * slots + slot_ids, -1).astype(jnp.float32)
        meta = jnp.concatenate([pos.T, gate_weights.T], axis=0)
        t2, mt = comm_call(
            spread_kernel, "spread", 1, [vmem, vmem],
            [jax.ShapeDtypeStruct((4, 4, rows, width), bf), jax.ShapeDtypeStruct((3, 4, 4, 16, rows), jnp.float32)],
            [dma((2, 3))] + [dma((3, 3))] * 4 + [dma((3, 4, 2))] * 2 + [dma((3, 4, 3))] * 2 + [dma((3, 4, 2))] * 2,
        )(tokens, meta)
        s = pl.pallas_call(
            lambda *refs: pick_kernel(slots, *refs),
            name="pick",
            grid=(4, 4),
            in_specs=[pl.BlockSpec((1, 1, rows, width), lambda a, b: (a, b, 0, 0)), pl.BlockSpec((3, 1, 1, 16, rows), lambda a, b: (0, a, b, 0, 0))],
            out_specs=pl.BlockSpec((4, 2, 1, 1, slots, width), lambda a, b: (0, 0, a, b, 0, 0)),
            out_shape=jax.ShapeDtypeStruct((4, 2, 4, 4, slots, width), bf),
        )(t2, mt)
        (r,) = comm_call(
            out_kernel, "send_out", 2, [hbm],
            [jax.ShapeDtypeStruct((2, 4, 4, 4, slots, width), bf)],
            [pltpu.VMEM((4, 4, slots, width), bf), dma((2, 3)), dma((3, 4, 2)), dma((3, 4, 2))],
        )(s)
        r = r.reshape(group_size * slots, width)
        proj_gate = jnp.dot(r, w_gate[0], preferred_element_type=jnp.float32)
        proj_up = jnp.dot(r, w_up[0], preferred_element_type=jnp.float32)
        hidden = (jax.nn.silu(proj_gate) * proj_up).astype(bf)
        y = jnp.dot(hidden, w_down[0], preferred_element_type=jnp.float32).astype(bf)
        y = y.reshape(2, 4, 4, 4, slots, width)
        z4, z5 = comm_call(
            back_kernel, "send_back", 3, [hbm],
            [jax.ShapeDtypeStruct((4, 2, 4, 4, slots, width), bf), jax.ShapeDtypeStruct((4, 4, 2, 4, slots, width), bf)],
            [pltpu.VMEM((4, 4, slots, width), bf), pltpu.VMEM((4, 2, 4, slots, width), bf), dma((4, 3)), dma((3, 4, 2)), dma((3, 4, 2)), dma((3, 3)), dma((3, 3))],
        )(y)
        part = pl.pallas_call(
            lambda *refs: weigh_kernel(slots, *refs),
            name="weigh",
            grid=(4,),
            in_specs=[pl.BlockSpec((4, 4, 2, 1, slots, width), lambda d: (0, 0, 0, d, 0, 0)), pl.BlockSpec((3, 4, 4, 16, rows), lambda d: (0, 0, 0, 0, 0))],
            out_specs=pl.BlockSpec((1, rows, width), lambda d: (d, 0, 0)),
            out_shape=jax.ShapeDtypeStruct((4, rows, width), jnp.float32),
        )(z5, mt)
        return comm_call(
            sum_kernel, "sum_up", 4, [hbm], jax.ShapeDtypeStruct((rows, width), bf),
            [pltpu.VMEM((4, rows, width), jnp.float32), dma((3,)), dma((3, 3)), dma((3, 3))],
        )(part)

    return jax.shard_map(local_layer, mesh=mesh, in_specs=(tok_spec, tok_spec, tok_spec, tok_spec, weight_spec, weight_spec, weight_spec), out_specs=tok_spec, check_vma=False)
```

```python
import jax
import jax.numpy as jnp
from jax import lax
from jax.experimental import pallas as pl
from jax.experimental.pallas import tpu as pltpu
from jax.sharding import PartitionSpec as P

MESH = pl.DeviceIdType.MESH
CAP_FACTOR = 2
RING = 4
DELTAS = (1, 3, 2)
COLS = ((0, 768), (768, 640), (1408, 640))
STRIDES = ((16, 4, 1), (4, 1, 16))


def capacity(rows, top_k, experts):
    return ((CAP_FACTOR * rows * top_k + 8 * experts - 1) // (8 * experts)) * 8


def place():
    core, e = lax.axis_index("node"), lax.axis_index("expert")
    z, y, x = e // 16, (e // 4) % 4, e % 4
    return core, e, ((z, y, x), (y, x, z))


def own_view(core, views):
    v = tuple(a + core * (b - a) for a, b in zip(*views))
    s = tuple(a + core * (b - a) for a, b in zip(*STRIDES))
    return v, s


def step(e, pos, stride, delta):
    return e + (lax.rem(pos + delta, RING) - pos) * stride


def cols(k):
    return pl.ds(*COLS[k])


def dims(k):
    return k % 3, (k + 1) % 3, (k + 2) % 3


def plane_at(k, d0, d1):
    return (d1, d0) if k == 2 else (d0, d1)


def cube_at(k, p):
    full = [slice(None)] * 3
    full[dims(k)[2]] = p
    return tuple(full)


def remote(src, dst, send, recv, core, e):
    return pltpu.make_async_remote_copy(src_ref=src, dst_ref=dst, send_sem=send, recv_sem=recv, device_id=(0, core, e), device_id_type=MESH)


def greet(targets):
    barrier = pltpu.get_barrier_semaphore()
    for core, e in targets:
        pl.semaphore_signal(barrier, inc=1, device_id=(0, core, e), device_id_type=MESH)
    pl.semaphore_wait(barrier, len(targets))


def ring_peers(core_list, e, views):
    out = []
    for core in core_list:
        for v, s in zip(views[0], STRIDES[0]):
            for delta in DELTAS:
                out.append((core, step(e, v, s, delta)))
    return out


def spread_kernel(tok, meta, t2, mt, loc, s1s, s1r, m1s, m1r, s2s, s2r, m2s, m2r, s3s, s3r):
    core, e, views = place()
    v, st = own_view(core, views)
    greet(ring_peers((core,), e, views))
    half = tok.shape[0] // 2
    sends, locals_ = [], []

    def go(copy):
        copy.start()
        sends.append(copy)

    for k in range(3):
        i0, i1, _ = dims(k)
        here = plane_at(k, v[i0], v[i1])
        for delta in DELTAS:
            peer = step(e, v[i0], st[i0], delta)
            go(remote(tok.at[:, cols(k)], t2.at[(*here, slice(None), cols(k))], s1s.at[k, delta - 1], s1r.at[k, delta - 1], core, peer))
            go(remote(meta, mt.at[(k, *here)], m1s.at[k, delta - 1], m1r.at[k, delta - 1], core, peer))
    for k in range(3):
        i0, i1, _ = dims(k)
        here = plane_at(k, v[i0], v[i1])
        own = pltpu.make_async_copy(tok.at[:, cols(k)], t2.at[(*here, slice(None), cols(k))], loc.at[0, k])
        own.start()
        locals_.append(own)
        own = pltpu.make_async_copy(meta, mt.at[(k, *here)], loc.at[1, k])
        own.start()
        locals_.append(own)

    def second(k, j):
        i0, i1, _ = dims(k)
        at = plane_at(k, lax.rem(v[i0] + j, RING), v[i1])
        block = t2.at[(*at, slice(None), cols(k))]
        for way, delta in enumerate((1, 3)):
            src = tok.at[:, cols(k)] if j == 0 else block
            go(remote(src, block, s2s.at[k, j, way], s2r.at[k, j, way], core, step(e, v[i1], st[i1], delta)))
        for delta in DELTAS:
            src = meta if j == 0 else mt.at[(k, *at)]
            go(remote(src, mt.at[(k, *at)], m2s.at[k, j, delta - 1], m2r.at[k, j, delta - 1], core, step(e, v[i1], st[i1], delta)))

    for k in range(3):
        second(k, 0)
    for j in DELTAS:
        for k in range(3):
            i0, i1, _ = dims(k)
            at = plane_at(k, lax.rem(v[i0] + j, RING), v[i1])
            block = t2.at[(*at, slice(None), cols(k))]
            remote(block, block, s1s.at[k, 3 - j], s1r.at[k, 3 - j], core, e).wait_recv()
            remote(mt.at[(k, *at)], mt.at[(k, *at)], m1s.at[k, 3 - j], m1r.at[k, 3 - j], core, e).wait_recv()
            second(k, j)
    for j in (0, *DELTAS):
        for k in range(3):
            i0, i1, _ = dims(k)
            for way, delta in enumerate((1, 3)):
                at = plane_at(k, lax.rem(v[i0] + j, RING), lax.rem(v[i1] + 4 - delta, RING))
                block = t2.at[(*at, slice(None), cols(k))]
                remote(block, block, s2s.at[k, j, way], s2r.at[k, j, way], core, e).wait_recv()
                part = t2.at[(*at, pl.ds(half * way, half), cols(k))]
                go(remote(part, part, s3s.at[k, j, way], s3r.at[k, j, way], core, step(e, v[i1], st[i1], delta)))
    for j in (0, *DELTAS):
        for k in range(3):
            i0, i1, _ = dims(k)
            for delta in DELTAS:
                at = plane_at(k, lax.rem(v[i0] + j, RING), lax.rem(v[i1] + 4 - delta, RING))
                remote(mt.at[(k, *at)], mt.at[(k, *at)], m2s.at[k, j, delta - 1], m2r.at[k, j, delta - 1], core, e).wait_recv()
            at = plane_at(k, lax.rem(v[i0] + j, RING), lax.rem(v[i1] + 2, RING))
            for way in range(2):
                part = t2.at[(*at, pl.ds(half * way, half), cols(k))]
                remote(part, part, s3s.at[k, j, way], s3r.at[k, j, way], core, e).wait_recv()
    for copy in sends:
        copy.wait_send()
    for copy in locals_:
        copy.wait()


def pick_kernel(slots, t2, mt, out):
    core, e, views = place()
    v, st = own_view(core, views)
    rows = RING * 2 * slots
    r = lax.broadcasted_iota(jnp.int32, (rows, 1), 0)
    p2, half, s = r // (2 * slots), (r // slots) % 2, r % slots
    for k in range(3):
        i0, i1, i2 = dims(k)
        key = ((half * 64 + v[i0] * st[i0] + v[i1] * st[i1] + p2 * st[i2]) * slots + s).astype(jnp.float32)
        hot = jnp.zeros((rows, t2.shape[2]), jnp.float32)
        for j in range(8):
            hot = jnp.where(key == mt[k, 0, 0, j:j + 1, :], 1.0, hot)
        got = jnp.dot(hot.astype(jnp.bfloat16), t2[0, 0, :, cols(k)], preferred_element_type=jnp.float32)
        out[:, :, 0, 0, :, cols(k)] = got.astype(jnp.bfloat16).reshape(RING, 2, slots, COLS[k][1])


def expert_kernel(slots, s_ref, wg_ref, wu_ref, wd_ref, z5, r, z4, wg, wu, wd, wsem, loc, s3, r3, s4, r4, s5, r5):
    core, e, views = place()
    v, st = own_view(core, views)
    other = own_view(1 - core, views)[0]
    part = slots // 2
    loads = [pltpu.make_async_copy(src.at[0], dst, wsem.at[i]) for i, (src, dst) in enumerate(((wg_ref, wg), (wu_ref, wu), (wd_ref, wd)))]
    for load in loads:
        load.start()
    greet(ring_peers((0, 1), e, views) + [(1 - core, e)])
    sends = []

    def go(copy):
        copy.start()
        sends.append(copy)

    def cube(q, o, k, p):
        return r.at[(q, o, *cube_at(k, p), slice(None), cols(k))]

    def inward(q, k):
        i2 = dims(k)[2]
        return pltpu.make_async_copy(s_ref.at[v[i2], core, :, :, pl.ds(part * q, part), cols(k)], cube(q, core, k, v[i2]), loc.at[0, q, k])

    for q in range(2):
        at = pl.ds(part * q, part)
        for delta in DELTAS:
            for k in range(3):
                i2 = dims(k)[2]
                for to in range(2):
                    go(remote(s_ref.at[lax.rem(v[i2] + delta, RING), to, :, :, at, cols(k)], cube(q, core, k, v[i2]), s3.at[q, k, delta, to], r3.at[q, k, delta, core], to, step(e, v[i2], st[i2], delta)))
        for k in range(3):
            i2 = dims(k)[2]
            go(remote(s_ref.at[v[i2], 1 - core, :, :, at, cols(k)], cube(q, core, k, v[i2]), s3.at[q, k, 0, 0], r3.at[q, k, 0, 0], 1 - core, e))
            inward(q, k).start()
    for load in loads:
        load.wait()

    def z4_at(q, k, p, c):
        return z4.at[q, p, c, :, :, :, cols(k)]

    def back(q, o, k, delta):
        i2 = dims(k)[2]
        here = views[o][i2]
        return remote(cube(q, o, k, lax.rem(here + delta, RING)), z4_at(q, k, here, core), s4.at[q, k, delta, o], r4.at[q, k, delta, core], o, step(e, here, STRIDES[o][i2], delta))

    def across(q, k):
        i2 = dims(k)[2]
        return remote(cube(q, 1 - core, k, other[i2]), z4_at(q, k, other[i2], core), s4.at[q, k, 0, 0], r4.at[q, k, 0, 0], 1 - core, e)

    def stay(q, k):
        i2 = dims(k)[2]
        return pltpu.make_async_copy(cube(q, core, k, v[i2]), z4_at(q, k, v[i2], core), loc.at[1, q, k])

    @pl.loop(0, 2)
    def _(q):
        for k in range(3):
            i2 = dims(k)[2]
            inward(q, k).wait()
            target = cube(q, 1 - core, k, other[i2])
            remote(target, target, s3.at[q, k, 0, 0], r3.at[q, k, 0, 0], core, e).wait_recv()
            for delta in DELTAS:
                for o in range(2):
                    target = cube(q, o, k, lax.rem(views[o][i2] + 4 - delta, RING))
                    remote(target, target, s3.at[q, k, delta, 0], r3.at[q, k, delta, o], core, e).wait_recv()
        for o in range(2):
            @pl.loop(0, RING)
            def _(i):
                x = r[q, o, i].reshape(RING * RING * part, r.shape[-1])
                gate = jnp.dot(x, wg[...], preferred_element_type=jnp.float32)
                up = jnp.dot(x, wu[...], preferred_element_type=jnp.float32)
                hidden = (jax.nn.silu(gate) * up).astype(jnp.bfloat16)
                y = jnp.dot(hidden, wd[...], preferred_element_type=jnp.float32).astype(jnp.bfloat16)
                r[q, o, i] = y.reshape(RING, RING, part, r.shape[-1])

            for delta in DELTAS:
                for k in range(3):
                    back(q, o, k, delta).start()
        for k in range(3):
            across(q, k).start()
            stay(q, k).start()

    def line(q, k, p):
        at = (slice(None), slice(None), p, slice(None)) if k == 2 else (slice(None), slice(None), slice(None), p)
        return z4.at[(q, *at, slice(None), cols(k))]

    keep = []
    for q in range(2):
        at = pl.ds(part * q, part)
        for k in range(3):
            i1, i2 = dims(k)[1:]
            stay(q, k).wait()
            target = z4_at(q, k, v[i2], 1 - core)
            remote(target, target, s4.at[q, k, 0, 0], r4.at[q, k, 0, 0], core, e).wait_recv()
            for delta in DELTAS:
                for o in range(2):
                    target = z4_at(q, k, lax.rem(v[i2] + 4 - delta, RING), o)
                    remote(target, target, s4.at[q, k, delta, 0], r4.at[q, k, delta, o], core, e).wait_recv()
            for delta in DELTAS:
                go(remote(line(q, k, lax.rem(v[i1] + delta, RING)), z5.at[v[i1], :, :, :, at, cols(k)], s5.at[q, k, delta - 1], r5.at[q, k, delta - 1], core, step(e, v[i1], st[i1], delta)))
            own = pltpu.make_async_copy(line(q, k, v[i1]), z5.at[v[i1], :, :, :, at, cols(k)], loc.at[2, q, k])
            own.start()
            keep.append(own)
    for own in keep:
        own.wait()
    for q in range(2):
        at = pl.ds(part * q, part)
        for k in range(3):
            i1 = dims(k)[1]
            for delta in DELTAS:
                target = z5.at[lax.rem(v[i1] + 4 - delta, RING), :, :, :, at, cols(k)]
                remote(target, target, s5.at[q, k, delta - 1], r5.at[q, k, delta - 1], core, e).wait_recv()
    for q in range(2):
        for k in range(3):
            across(q, k).wait_send()
            for delta in DELTAS:
                for o in range(2):
                    back(q, o, k, delta).wait_send()
    for copy in sends:
        copy.wait_send()


def sum_kernel(slots, z5, mt, out, zb, part, q, load, own_sem, ss, rs):
    core, e, views = place()
    v, st = own_view(core, views)
    n = RING * RING * 2 * slots
    def fetch(turn, k):
        i0 = dims(k)[0]
        h = turn // 2
        delta = (1 - h) * (2 - turn) + h * (9 - 3 * turn)
        d0 = lax.rem(v[i0] + delta, RING)
        return delta, pltpu.make_async_copy(z5.at[:, :, :, d0, :, cols(k)], zb.at[lax.rem(turn, 2), :, :, :, :, cols(k)], load.at[lax.rem(turn, 2), k])

    def push(delta, k):
        i0 = dims(k)[0]
        return remote(part.at[delta, :, cols(k)], q.at[delta - 1, :, cols(k)], ss.at[k, delta - 1], rs.at[k, delta - 1], core, step(e, v[i0], st[i0], delta))

    for k in range(3):
        fetch(0, k)[1].start()
    greet(ring_peers((core,), e, views))
    r = lax.broadcasted_iota(jnp.int32, (1, n), 1)
    d1, p2, half, s = r // (RING * 2 * slots), (r // (2 * slots)) % RING, (r // slots) % 2, r % slots

    @pl.loop(0, 4)
    def _(turn):
        @pl.when(turn < 3)
        def _():
            for k in range(3):
                fetch(turn + 1, k)[1].start()

        for k in range(3):
            delta, copy = fetch(turn, k)
            copy.wait()
            i0, i1, i2 = dims(k)
            a, b = plane_at(k, lax.rem(v[i0] + delta, RING), v[i1])
            m = jnp.transpose(mt[k, a, b])
            key = ((half * 64 + v[i0] * st[i0] + d1 * st[i1] + p2 * st[i2]) * slots + s).astype(jnp.float32)
            w = jnp.zeros((m.shape[0], n), jnp.float32)
            for j in range(8):
                w = jnp.where(m[:, j:j + 1] == key, m[:, 8 + j:9 + j], w)
            hi = w.astype(jnp.bfloat16)
            rest = w - hi.astype(jnp.float32)
            mid = rest.astype(jnp.bfloat16)
            low = (rest - mid.astype(jnp.float32)).astype(jnp.bfloat16)
            y = zb[lax.rem(turn, 2), :, :, :, :, cols(k)].reshape(n, COLS[k][1])
            total = jnp.dot(low, y, preferred_element_type=jnp.float32)
            total += jnp.dot(mid, y, preferred_element_type=jnp.float32)
            total += jnp.dot(hi, y, preferred_element_type=jnp.float32)
            part[delta, :, cols(k)] = total

            @pl.when(turn < 3)
            def _():
                push(delta, k).start()

    for delta in DELTAS:
        for k in range(3):
            target = q.at[delta - 1, :, cols(k)]
            remote(target, target, ss.at[k, delta - 1], rs.at[k, delta - 1], core, e).wait_recv()

    @pl.loop(0, out.shape[0] // 16)
    def _(i):
        at = pl.ds(pl.multiple_of(i * 16, 16), 16)
        out[at, :] = ((part[0, at, :] + q[0, at, :]) + (q[1, at, :] + q[2, at, :])).astype(jnp.bfloat16)

    for delta in DELTAS:
        for k in range(3):
            push(delta, k).wait_send()


def comm_call(body, name, cid, ins, outs, scratch):
    return pl.pallas_call(
        body,
        name=name,
        out_shape=outs,
        in_specs=ins,
        out_specs=[pl.BlockSpec(memory_space=pltpu.HBM)] * len(outs) if isinstance(outs, list) else pl.BlockSpec(memory_space=pltpu.VMEM),
        scratch_shapes=scratch,
        compiler_params=pltpu.CompilerParams(collective_id=cid, has_side_effects=True),
    )


def solution(mesh):
    group_axes = ("node", "expert")
    group_size = mesh.shape["node"] * mesh.shape["expert"]
    tok_spec = P(("data", "node", "expert"), None)
    weight_spec = P(("node", "expert"), None, None)
    hbm = pl.BlockSpec(memory_space=pltpu.HBM)
    vmem = pl.BlockSpec(memory_space=pltpu.VMEM)
    dma = pltpu.SemaphoreType.DMA

    def local_layer(tokens, expert_ids, gate_weights, slot_ids, w_gate, w_up, w_down):
        rows, width = tokens.shape
        top_k = expert_ids.shape[1]
        slots = capacity(rows, top_k, group_size)
        bf = jnp.bfloat16
        pos = jnp.where(slot_ids >= 0, expert_ids * slots + slot_ids, -1).astype(jnp.float32)
        meta = jnp.concatenate([pos.T, gate_weights.T], axis=0)
        t2, mt = comm_call(
            spread_kernel, "spread", 1, [vmem, vmem],
            [jax.ShapeDtypeStruct((4, 4, rows, width), bf), jax.ShapeDtypeStruct((3, 4, 4, 16, rows), jnp.float32)],
            [dma((2, 3))] + [dma((3, 3))] * 4 + [dma((3, 4, 2))] * 2 + [dma((3, 4, 3))] * 2 + [dma((3, 4, 2))] * 2,
        )(tokens, meta)
        s = pl.pallas_call(
            lambda *refs: pick_kernel(slots, *refs),
            name="pick",
            grid=(4, 4),
            in_specs=[pl.BlockSpec((1, 1, rows, width), lambda a, b: (a, b, 0, 0)), pl.BlockSpec((3, 1, 1, 16, rows), lambda a, b: (0, a, b, 0, 0))],
            out_specs=pl.BlockSpec((4, 2, 1, 1, slots, width), lambda a, b: (0, 0, a, b, 0, 0)),
            out_shape=jax.ShapeDtypeStruct((4, 2, 4, 4, slots, width), bf),
        )(t2, mt)
        (z5,) = comm_call(
            lambda *refs: expert_kernel(slots, *refs), "experts", 2, [hbm] * 4,
            [jax.ShapeDtypeStruct((4, 4, 2, 4, slots, width), bf)],
            [pltpu.VMEM((2, 2, 4, 4, 4, slots // 2, width), bf), pltpu.VMEM((2, 4, 2, 4, 4, slots // 2, width), bf)]
            + [pltpu.VMEM(w.shape[1:], bf) for w in (w_gate, w_up, w_down)]
            + [dma((3,)), dma((3, 2, 3))] + [dma((2, 3, 4, 2))] * 4 + [dma((2, 3, 3))] * 2,
        )(s, w_gate, w_up, w_down)
        return comm_call(
            lambda *refs: sum_kernel(slots, *refs), "weigh_sum", 4, [hbm, vmem], jax.ShapeDtypeStruct((rows, width), bf),
            [pltpu.VMEM((2, 4, 4, 2, slots, width), bf), pltpu.VMEM((4, rows, width), jnp.float32), pltpu.VMEM((3, rows, width), jnp.float32), dma((2, 3)), dma((3,)), dma((3, 3)), dma((3, 3))],
        )(z5, mt)

    return jax.shard_map(local_layer, mesh=mesh, in_specs=(tok_spec, tok_spec, tok_spec, tok_spec, weight_spec, weight_spec, weight_spec), out_specs=tok_spec, check_vma=False)
```

```python
import jax
import jax.numpy as jnp
from jax import lax
from jax.experimental import pallas as pl
from jax.experimental.pallas import tpu as pltpu
from jax.sharding import PartitionSpec as P

MESH = pl.DeviceIdType.MESH
CAP_FACTOR = 2
RING = 4
DELTAS = (1, 3, 2)
COLS = ((0, 768), (768, 640), (1408, 640))
STRIDES = ((16, 4, 1), (4, 1, 16))


def capacity(rows, top_k, experts):
    return ((CAP_FACTOR * rows * top_k + 8 * experts - 1) // (8 * experts)) * 8


def place():
    core, e = lax.axis_index("node"), lax.axis_index("expert")
    z, y, x = e // 16, (e // 4) % 4, e % 4
    return core, e, ((z, y, x), (y, x, z))


def own_view(core, views):
    v = tuple(a + core * (b - a) for a, b in zip(*views))
    s = tuple(a + core * (b - a) for a, b in zip(*STRIDES))
    return v, s


def step(e, pos, stride, delta):
    return e + (lax.rem(pos + delta, RING) - pos) * stride


def cols(k):
    return pl.ds(*COLS[k])


def dims(k):
    return k % 3, (k + 1) % 3, (k + 2) % 3


def plane_at(k, d0, d1):
    return (d1, d0) if k == 2 else (d0, d1)


def cube_at(k, p):
    full = [slice(None)] * 3
    full[dims(k)[2]] = p
    return tuple(full)


def remote(src, dst, send, recv, core, e):
    return pltpu.make_async_remote_copy(src_ref=src, dst_ref=dst, send_sem=send, recv_sem=recv, device_id=(0, core, e), device_id_type=MESH)


def greet(targets):
    barrier = pltpu.get_barrier_semaphore()
    for core, e in targets:
        pl.semaphore_signal(barrier, inc=1, device_id=(0, core, e), device_id_type=MESH)
    pl.semaphore_wait(barrier, len(targets))


def ring_peers(core_list, e, views):
    out = []
    for core in core_list:
        for v, s in zip(views[0], STRIDES[0]):
            for delta in DELTAS:
                out.append((core, step(e, v, s, delta)))
    return out


def spread_kernel(slots, tok, meta, s_ref, mt, t2, tile0, tile1, tile2, loc, out_sem, s1s, s1r, m1s, m1r, s2s, s2r, m2s, m2r, s3s, s3r):
    core, e, views = place()
    v, st = own_view(core, views)
    greet(ring_peers((core,), e, views))
    rows = tok.shape[0]
    tiles = (tile0, tile1, tile2)

    def at(k, j0, j1):
        i0, i1, _ = dims(k)
        return plane_at(k, lax.rem(v[i0] + j0, RING), lax.rem(v[i1] + j1, RING))

    def block(k, j0, j1):
        return t2.at[(*at(k, j0, j1), slice(None), cols(k))]

    def info(k, j0, j1):
        return mt.at[(k, *at(k, j0, j1))]

    def first(k, delta):
        i0 = dims(k)[0]
        peer = step(e, v[i0], st[i0], delta)
        return (remote(tok.at[:, cols(k)], block(k, 0, 0), s1s.at[k, delta - 1], s1r.at[k, delta - 1], core, peer),
                remote(meta, info(k, 0, 0), m1s.at[k, delta - 1], m1r.at[k, delta - 1], core, peer))

    def second(k, j, way):
        i1 = dims(k)[1]
        return remote(block(k, j, 0), block(k, j, 0), s2s.at[k, j, way], s2r.at[k, j, way], core, step(e, v[i1], st[i1], 1 + 2 * way))

    def second_info(k, j, delta):
        i1 = dims(k)[1]
        return remote(info(k, j, 0), info(k, j, 0), m2s.at[k, j, delta - 1], m2r.at[k, j, delta - 1], core, step(e, v[i1], st[i1], delta))

    def third(k, j, way):
        i1 = dims(k)[1]
        piece = t2.at[(*at(k, j, 3 - 2 * way), pl.ds(rows // 2 * way, rows // 2), cols(k))]
        return remote(piece, piece, s3s.at[k, j, way], s3r.at[k, j, way], core, step(e, v[i1], st[i1], 1 + 2 * way))

    def second_all(k, j):
        for way in range(2):
            second(k, j, way).start()
        for delta in DELTAS:
            second_info(k, j, delta).start()

    def keep(k):
        return pltpu.make_async_copy(tok.at[:, cols(k)], block(k, 0, 0), loc.at[0, k]), pltpu.make_async_copy(meta, info(k, 0, 0), loc.at[1, k])

    def put(k, n, j0, j1):
        return pltpu.make_async_copy(tiles[k].at[lax.rem(n, 2)], s_ref.at[(slice(None), slice(None), *at(k, j0, j1), slice(None), cols(k))], out_sem.at[k, lax.rem(n, 2)])

    def pick(k, n, j0, j1):
        i0, i1, i2 = dims(k)
        total = RING * 2 * slots
        r = lax.broadcasted_iota(jnp.int32, (total, 1), 0)
        p2, half, s = r // (2 * slots), (r // slots) % 2, r % slots
        key = ((half * 64 + v[i0] * st[i0] + v[i1] * st[i1] + p2 * st[i2]) * slots + s).astype(jnp.float32)
        a, b = at(k, j0, j1)
        hot = jnp.zeros((total, rows), jnp.float32)
        for j in range(8):
            hot = jnp.where(key == mt[k, a, b, j:j + 1, :], 1.0, hot)
        got = jnp.dot(hot.astype(jnp.bfloat16), t2[a, b, :, cols(k)], preferred_element_type=jnp.float32)

        @pl.when(n >= 2)
        def _():
            put(k, n, j0, j1).wait()

        tiles[k][lax.rem(n, 2)] = got.astype(jnp.bfloat16).reshape(RING, 2, slots, COLS[k][1])
        put(k, n, j0, j1).start()

    def gray(t):
        return t + (t // 2) * (5 - 2 * t)

    for k in range(3):
        for copy in keep(k):
            copy.start()
    for delta in (2, 1, 3):
        for k in range(3):
            for copy in first(k, delta):
                copy.start()
    for k in range(3):
        for copy in keep(k):
            copy.wait()
        second_all(k, 0)
    for j in DELTAS:
        for k in range(3):
            remote(block(k, j, 0), block(k, j, 0), s1s.at[k, 3 - j], s1r.at[k, 3 - j], core, e).wait_recv()
            remote(info(k, j, 0), info(k, j, 0), m1s.at[k, 3 - j], m1r.at[k, 3 - j], core, e).wait_recv()
            second_all(k, j)

    @pl.loop(0, RING)
    def _(t):
        j = gray(t)
        for k in range(3):
            for way in range(2):
                came = block(k, j, 3 - 2 * way)
                remote(came, came, s2s.at[k, j, way], s2r.at[k, j, way], core, e).wait_recv()
                third(k, j, way).start()
            for delta in (1, 3):
                came = info(k, j, 4 - delta)
                remote(came, came, m2s.at[k, j, delta - 1], m2r.at[k, j, delta - 1], core, e).wait_recv()

        @pl.loop(0, 3)
        def _(d):
            for k in range(3):
                pick(k, t * 3 + d, j, d + d // 2)

    @pl.loop(0, RING)
    def _(t):
        j = gray(t)
        for k in range(3):
            for way in range(2):
                came = t2.at[(*at(k, j, 2), pl.ds(rows // 2 * way, rows // 2), cols(k))]
                remote(came, came, s3s.at[k, j, way], s3r.at[k, j, way], core, e).wait_recv()
            came = info(k, j, 2)
            remote(came, came, m2s.at[k, j, 1], m2r.at[k, j, 1], core, e).wait_recv()
            pick(k, 12 + t, j, 2)

    for k in range(3):
        for n in range(2):
            put(k, n, 0, 0).wait()
        for delta in DELTAS:
            for copy in first(k, delta):
                copy.wait_send()
        for j in range(RING):
            for way in range(2):
                second(k, j, way).wait_send()
                third(k, j, way).wait_send()
            for delta in DELTAS:
                second_info(k, j, delta).wait_send()


def expert_kernel(slots, s_ref, wg_ref, wu_ref, wd_ref, z5, r, z4, wg, wu, wd, wsem, loc, s3, r3, s4, r4, s5, r5):
    core, e, views = place()
    v, st = own_view(core, views)
    other = own_view(1 - core, views)[0]
    part = slots // 2
    loads = [pltpu.make_async_copy(src.at[0], dst, wsem.at[i]) for i, (src, dst) in enumerate(((wg_ref, wg), (wu_ref, wu), (wd_ref, wd)))]
    for load in loads:
        load.start()
    greet(ring_peers((0, 1), e, views) + [(1 - core, e)])
    sends = []

    def go(copy):
        copy.start()
        sends.append(copy)

    def cube(q, o, k, p):
        return r.at[(q, o, *cube_at(k, p), slice(None), cols(k))]

    def inward(q, k):
        i2 = dims(k)[2]
        return pltpu.make_async_copy(s_ref.at[v[i2], core, :, :, pl.ds(part * q, part), cols(k)], cube(q, core, k, v[i2]), loc.at[0, q, k])

    for q in range(2):
        at = pl.ds(part * q, part)
        for delta in DELTAS:
            for k in range(3):
                i2 = dims(k)[2]
                for to in range(2):
                    go(remote(s_ref.at[lax.rem(v[i2] + delta, RING), to, :, :, at, cols(k)], cube(q, core, k, v[i2]), s3.at[q, k, delta, to], r3.at[q, k, delta, core], to, step(e, v[i2], st[i2], delta)))
        for k in range(3):
            i2 = dims(k)[2]
            go(remote(s_ref.at[v[i2], 1 - core, :, :, at, cols(k)], cube(q, core, k, v[i2]), s3.at[q, k, 0, 0], r3.at[q, k, 0, 0], 1 - core, e))
            inward(q, k).start()
    for load in loads:
        load.wait()

    def z4_at(q, k, p, c):
        return z4.at[q, p, c, :, :, :, cols(k)]

    def back(q, o, k, delta):
        i2 = dims(k)[2]
        here = views[o][i2]
        return remote(cube(q, o, k, lax.rem(here + delta, RING)), z4_at(q, k, here, core), s4.at[q, k, delta, o], r4.at[q, k, delta, core], o, step(e, here, STRIDES[o][i2], delta))

    def across(q, k):
        i2 = dims(k)[2]
        return remote(cube(q, 1 - core, k, other[i2]), z4_at(q, k, other[i2], core), s4.at[q, k, 0, 0], r4.at[q, k, 0, 0], 1 - core, e)

    def stay(q, k):
        i2 = dims(k)[2]
        return pltpu.make_async_copy(cube(q, core, k, v[i2]), z4_at(q, k, v[i2], core), loc.at[1, q, k])

    @pl.loop(0, 2)
    def _(q):
        for k in range(3):
            i2 = dims(k)[2]
            inward(q, k).wait()
            target = cube(q, 1 - core, k, other[i2])
            remote(target, target, s3.at[q, k, 0, 0], r3.at[q, k, 0, 0], core, e).wait_recv()
            for delta in DELTAS:
                for o in range(2):
                    target = cube(q, o, k, lax.rem(views[o][i2] + 4 - delta, RING))
                    remote(target, target, s3.at[q, k, delta, 0], r3.at[q, k, delta, o], core, e).wait_recv()
        for o in range(2):
            @pl.loop(0, RING)
            def _(i):
                x = r[q, o, i].reshape(RING * RING * part, r.shape[-1])
                gate = jnp.dot(x, wg[...], preferred_element_type=jnp.float32)
                up = jnp.dot(x, wu[...], preferred_element_type=jnp.float32)
                hidden = (jax.nn.silu(gate) * up).astype(jnp.bfloat16)
                y = jnp.dot(hidden, wd[...], preferred_element_type=jnp.float32).astype(jnp.bfloat16)
                r[q, o, i] = y.reshape(RING, RING, part, r.shape[-1])

            for delta in DELTAS:
                for k in range(3):
                    back(q, o, k, delta).start()
        for k in range(3):
            across(q, k).start()
            stay(q, k).start()

    def line(q, k, p):
        at = (slice(None), slice(None), p, slice(None)) if k == 2 else (slice(None), slice(None), slice(None), p)
        return z4.at[(q, *at, slice(None), cols(k))]

    keep = []
    for q in range(2):
        at = pl.ds(part * q, part)
        for k in range(3):
            i1, i2 = dims(k)[1:]
            stay(q, k).wait()
            target = z4_at(q, k, v[i2], 1 - core)
            remote(target, target, s4.at[q, k, 0, 0], r4.at[q, k, 0, 0], core, e).wait_recv()
            for delta in DELTAS:
                for o in range(2):
                    target = z4_at(q, k, lax.rem(v[i2] + 4 - delta, RING), o)
                    remote(target, target, s4.at[q, k, delta, 0], r4.at[q, k, delta, o], core, e).wait_recv()
            for delta in DELTAS:
                go(remote(line(q, k, lax.rem(v[i1] + delta, RING)), z5.at[v[i1], :, :, :, at, cols(k)], s5.at[q, k, delta - 1], r5.at[q, k, delta - 1], core, step(e, v[i1], st[i1], delta)))
            own = pltpu.make_async_copy(line(q, k, v[i1]), z5.at[v[i1], :, :, :, at, cols(k)], loc.at[2, q, k])
            own.start()
            keep.append(own)
    for own in keep:
        own.wait()
    for q in range(2):
        at = pl.ds(part * q, part)
        for k in range(3):
            i1 = dims(k)[1]
            for delta in DELTAS:
                target = z5.at[lax.rem(v[i1] + 4 - delta, RING), :, :, :, at, cols(k)]
                remote(target, target, s5.at[q, k, delta - 1], r5.at[q, k, delta - 1], core, e).wait_recv()
    for q in range(2):
        for k in range(3):
            across(q, k).wait_send()
            for delta in DELTAS:
                for o in range(2):
                    back(q, o, k, delta).wait_send()
    for copy in sends:
        copy.wait_send()


def sum_kernel(slots, z5, mt, out, zb, part, q, load, own_sem, ss, rs):
    core, e, views = place()
    v, st = own_view(core, views)
    n = RING * RING * 2 * slots
    def fetch(turn, k):
        i0 = dims(k)[0]
        h = turn // 2
        delta = (1 - h) * (2 - turn) + h * (9 - 3 * turn)
        d0 = lax.rem(v[i0] + delta, RING)
        return delta, pltpu.make_async_copy(z5.at[:, :, :, d0, :, cols(k)], zb.at[lax.rem(turn, 2), :, :, :, :, cols(k)], load.at[lax.rem(turn, 2), k])

    def push(delta, k):
        i0 = dims(k)[0]
        return remote(part.at[delta, :, cols(k)], q.at[delta - 1, :, cols(k)], ss.at[k, delta - 1], rs.at[k, delta - 1], core, step(e, v[i0], st[i0], delta))

    for k in range(3):
        fetch(0, k)[1].start()
    greet(ring_peers((core,), e, views))
    r = lax.broadcasted_iota(jnp.int32, (1, n), 1)
    d1, p2, half, s = r // (RING * 2 * slots), (r // (2 * slots)) % RING, (r // slots) % 2, r % slots

    @pl.loop(0, 4)
    def _(turn):
        @pl.when(turn < 3)
        def _():
            for k in range(3):
                fetch(turn + 1, k)[1].start()

        for k in range(3):
            delta, copy = fetch(turn, k)
            copy.wait()
            i0, i1, i2 = dims(k)
            a, b = plane_at(k, lax.rem(v[i0] + delta, RING), v[i1])
            m = jnp.transpose(mt[k, a, b])
            key = ((half * 64 + v[i0] * st[i0] + d1 * st[i1] + p2 * st[i2]) * slots + s).astype(jnp.float32)
            w = jnp.zeros((m.shape[0], n), jnp.float32)
            for j in range(8):
                w = jnp.where(m[:, j:j + 1] == key, m[:, 8 + j:9 + j], w)
            hi = w.astype(jnp.bfloat16)
            rest = w - hi.astype(jnp.float32)
            mid = rest.astype(jnp.bfloat16)
            low = (rest - mid.astype(jnp.float32)).astype(jnp.bfloat16)
            y = zb[lax.rem(turn, 2), :, :, :, :, cols(k)].reshape(n, COLS[k][1])
            total = jnp.dot(low, y, preferred_element_type=jnp.float32)
            total += jnp.dot(mid, y, preferred_element_type=jnp.float32)
            total += jnp.dot(hi, y, preferred_element_type=jnp.float32)
            part[delta, :, cols(k)] = total

            @pl.when(turn < 3)
            def _():
                push(delta, k).start()

    for delta in DELTAS:
        for k in range(3):
            target = q.at[delta - 1, :, cols(k)]
            remote(target, target, ss.at[k, delta - 1], rs.at[k, delta - 1], core, e).wait_recv()

    @pl.loop(0, out.shape[0] // 16)
    def _(i):
        at = pl.ds(pl.multiple_of(i * 16, 16), 16)
        out[at, :] = ((part[0, at, :] + q[0, at, :]) + (q[1, at, :] + q[2, at, :])).astype(jnp.bfloat16)

    for delta in DELTAS:
        for k in range(3):
            push(delta, k).wait_send()


def comm_call(body, name, cid, ins, outs, scratch):
    return pl.pallas_call(
        body,
        name=name,
        out_shape=outs,
        in_specs=ins,
        out_specs=[pl.BlockSpec(memory_space=pltpu.HBM)] * len(outs) if isinstance(outs, list) else pl.BlockSpec(memory_space=pltpu.VMEM),
        scratch_shapes=scratch,
        compiler_params=pltpu.CompilerParams(collective_id=cid, has_side_effects=True),
    )


def solution(mesh):
    group_axes = ("node", "expert")
    group_size = mesh.shape["node"] * mesh.shape["expert"]
    tok_spec = P(("data", "node", "expert"), None)
    weight_spec = P(("node", "expert"), None, None)
    hbm = pl.BlockSpec(memory_space=pltpu.HBM)
    vmem = pl.BlockSpec(memory_space=pltpu.VMEM)
    dma = pltpu.SemaphoreType.DMA

    def local_layer(tokens, expert_ids, gate_weights, slot_ids, w_gate, w_up, w_down):
        rows, width = tokens.shape
        top_k = expert_ids.shape[1]
        slots = capacity(rows, top_k, group_size)
        bf = jnp.bfloat16
        pos = jnp.where(slot_ids >= 0, expert_ids * slots + slot_ids, -1).astype(jnp.float32)
        meta = jnp.concatenate([pos.T, gate_weights.T], axis=0)
        s, mt = pl.pallas_call(
            lambda *refs: spread_kernel(slots, *refs),
            name="spread",
            in_specs=[vmem, vmem],
            out_specs=[hbm, vmem],
            out_shape=[jax.ShapeDtypeStruct((4, 2, 4, 4, slots, width), bf), jax.ShapeDtypeStruct((3, 4, 4, 16, rows), jnp.float32)],
            scratch_shapes=[pltpu.VMEM((4, 4, rows, width), bf)] + [pltpu.VMEM((2, 4, 2, slots, n), bf) for _, n in COLS]
            + [dma((2, 3)), dma((3, 2))] + [dma((3, 3))] * 4 + [dma((3, 4, 2))] * 2 + [dma((3, 4, 3))] * 2 + [dma((3, 4, 2))] * 2,
            compiler_params=pltpu.CompilerParams(collective_id=1, has_side_effects=True),
        )(tokens, meta)
        (z5,) = comm_call(
            lambda *refs: expert_kernel(slots, *refs), "experts", 2, [hbm] * 4,
            [jax.ShapeDtypeStruct((4, 4, 2, 4, slots, width), bf)],
            [pltpu.VMEM((2, 2, 4, 4, 4, slots // 2, width), bf), pltpu.VMEM((2, 4, 2, 4, 4, slots // 2, width), bf)]
            + [pltpu.VMEM(w.shape[1:], bf) for w in (w_gate, w_up, w_down)]
            + [dma((3,)), dma((3, 2, 3))] + [dma((2, 3, 4, 2))] * 4 + [dma((2, 3, 3))] * 2,
        )(s, w_gate, w_up, w_down)
        return comm_call(
            lambda *refs: sum_kernel(slots, *refs), "weigh_sum", 4, [hbm, vmem], jax.ShapeDtypeStruct((rows, width), bf),
            [pltpu.VMEM((2, 4, 4, 2, slots, width), bf), pltpu.VMEM((4, rows, width), jnp.float32), pltpu.VMEM((3, rows, width), jnp.float32), dma((2, 3)), dma((3,)), dma((3, 3)), dma((3, 3))],
        )(z5, mt)

    return jax.shard_map(local_layer, mesh=mesh, in_specs=(tok_spec, tok_spec, tok_spec, tok_spec, weight_spec, weight_spec, weight_spec), out_specs=tok_spec, check_vma=False)
```

```python
import jax
import jax.numpy as jnp
from jax import lax
from jax.experimental import pallas as pl
from jax.experimental.pallas import tpu as pltpu
from jax.sharding import PartitionSpec as P

MESH = pl.DeviceIdType.MESH
CAP_FACTOR = 2
RING = 4
DELTAS = (1, 3, 2)
COLS = ((0, 768), (768, 640), (1408, 640))
STRIDES = ((16, 4, 1), (4, 1, 16))


def capacity(rows, top_k, experts):
    return ((CAP_FACTOR * rows * top_k + 8 * experts - 1) // (8 * experts)) * 8


def place():
    core, e = lax.axis_index("node"), lax.axis_index("expert")
    z, y, x = e // 16, (e // 4) % 4, e % 4
    return core, e, ((z, y, x), (y, x, z))


def own_view(core, views):
    v = tuple(a + core * (b - a) for a, b in zip(*views))
    s = tuple(a + core * (b - a) for a, b in zip(*STRIDES))
    return v, s


def step(e, pos, stride, delta):
    return e + (lax.rem(pos + delta, RING) - pos) * stride


def cols(k):
    return pl.ds(*COLS[k])


def dims(k):
    return k % 3, (k + 1) % 3, (k + 2) % 3


def plane_at(k, d0, d1):
    return (d1, d0) if k == 2 else (d0, d1)


def cube_at(k, p):
    full = [slice(None)] * 3
    full[dims(k)[2]] = p
    return tuple(full)


def remote(src, dst, send, recv, core, e):
    return pltpu.make_async_remote_copy(src_ref=src, dst_ref=dst, send_sem=send, recv_sem=recv, device_id=(0, core, e), device_id_type=MESH)


def greet(targets):
    barrier = pltpu.get_barrier_semaphore()
    for core, e in targets:
        pl.semaphore_signal(barrier, inc=1, device_id=(0, core, e), device_id_type=MESH)
    pl.semaphore_wait(barrier, len(targets))


def ring_peers(core_list, e, views):
    out = []
    for core in core_list:
        for v, s in zip(views[0], STRIDES[0]):
            for delta in DELTAS:
                out.append((core, step(e, v, s, delta)))
    return out


def layer_kernel(slots, tok, meta, wg_ref, wu_ref, wd_ref, s_ref, z4, z5, own, came2, mt, t2, tile0, tile1, tile2, r, bounce, wg, wu, wd, sums, passing,
                 loc0, out_sem, s1s, s1r, m1s, m1r, s2s, s2r, m2s, m2r, s3s, s3r, wsem, loc, xes, xer, xs, xr, s4, r4, s5, r5,
                 relay_s, relay_r, load_sem, hs, hr, ps, pr):
    core, e, views = place()
    v, st = own_view(core, views)
    other = own_view(1 - core, views)[0]
    half_slots = slots // 2
    loads = [pltpu.make_async_copy(src.at[0], dst, wsem.at[i]) for i, (src, dst) in enumerate(((wg_ref, wg), (wu_ref, wu), (wd_ref, wd)))]
    greet(ring_peers((0, 1), e, views) + [(1 - core, e)])
    rows = tok.shape[0]
    tiles = (tile0, tile1, tile2)

    def at(k, j0, j1):
        i0, i1, _ = dims(k)
        return plane_at(k, lax.rem(v[i0] + j0, RING), lax.rem(v[i1] + j1, RING))

    def block(k, j0, j1):
        return t2.at[(*at(k, j0, j1), slice(None), cols(k))]

    def info(k, j0, j1):
        return mt.at[(k, *at(k, j0, j1))]

    def first(k, delta):
        i0 = dims(k)[0]
        return remote(tok.at[:, cols(k)], block(k, 0, 0), s1s.at[k, delta - 1], s1r.at[k, delta - 1], core, step(e, v[i0], st[i0], delta))

    def first_info(k, delta):
        i0 = dims(k)[0]
        return remote(meta, info(k, 0, 0), m1s.at[k, delta - 1], m1r.at[k, delta - 1], core, step(e, v[i0], st[i0], delta))

    def relay(k, way):
        i0 = dims(k)[0]
        piece = t2.at[(*at(k, 3 - 2 * way, 0), pl.ds(rows // 2 * way, rows // 2), cols(k))]
        return remote(piece, piece, relay_s.at[k, way], relay_r.at[k, way], core, step(e, v[i0], st[i0], 1 + 2 * way))

    def second(k, j, way):
        i1 = dims(k)[1]
        return remote(block(k, j, 0), block(k, j, 0), s2s.at[k, j, way], s2r.at[k, j, way], core, step(e, v[i1], st[i1], 1 + 2 * way))

    def second_info(k, j, delta):
        i1 = dims(k)[1]
        return remote(info(k, j, 0), info(k, j, 0), m2s.at[k, j, delta - 1], m2r.at[k, j, delta - 1], core, step(e, v[i1], st[i1], delta))

    def third(k, j, way):
        i1 = dims(k)[1]
        piece = t2.at[(*at(k, j, 3 - 2 * way), pl.ds(rows // 2 * way, rows // 2), cols(k))]
        return remote(piece, piece, s3s.at[k, j, way], s3r.at[k, j, way], core, step(e, v[i1], st[i1], 1 + 2 * way))

    def second_all(k, j):
        for way in range(2):
            second(k, j, way).start()
        for delta in DELTAS:
            second_info(k, j, delta).start()

    def keep(k):
        return pltpu.make_async_copy(tok.at[:, cols(k)], block(k, 0, 0), loc0.at[0, k]), pltpu.make_async_copy(meta, info(k, 0, 0), loc0.at[1, k])

    def put(k, n, j0, j1):
        return pltpu.make_async_copy(tiles[k].at[lax.rem(n, 2)], s_ref.at[(slice(None), slice(None), *at(k, j0, j1), slice(None), cols(k))], out_sem.at[k, lax.rem(n, 2)])

    def pick(k, n, j0, j1):
        i0, i1, i2 = dims(k)
        total = RING * 2 * slots
        r = lax.broadcasted_iota(jnp.int32, (total, 1), 0)
        p2, half, s = r // (2 * slots), (r // slots) % 2, r % slots
        key = ((half * 64 + v[i0] * st[i0] + v[i1] * st[i1] + p2 * st[i2]) * slots + s).astype(jnp.float32)
        a, b = at(k, j0, j1)
        hot = jnp.zeros((total, rows), jnp.float32)
        for j in range(8):
            hot = jnp.where(key == mt[k, a, b, j:j + 1, :], 1.0, hot)
        got = jnp.dot(hot.astype(jnp.bfloat16), t2[a, b, :, cols(k)], preferred_element_type=jnp.float32)

        @pl.when(n >= 2)
        def _():
            put(k, n, j0, j1).wait()

        tiles[k][lax.rem(n, 2)] = got.astype(jnp.bfloat16).reshape(RING, 2, slots, COLS[k][1])
        put(k, n, j0, j1).start()

    def gray(t):
        return t + (t // 2) * (5 - 2 * t)

    for k in range(3):
        for copy in keep(k):
            copy.start()
    for delta in DELTAS:
        for k in range(3):
            if delta != 2:
                first(k, delta).start()
            first_info(k, delta).start()
    for k in range(3):
        for copy in keep(k):
            copy.wait()
        second_all(k, 0)
    for j in DELTAS:
        for k in range(3):
            if j == 2:
                for way in range(2):
                    piece = t2.at[(*at(k, 2, 0), pl.ds(rows // 2 * way, rows // 2), cols(k))]
                    remote(piece, piece, relay_s.at[k, way], relay_r.at[k, way], core, e).wait_recv()
            else:
                remote(block(k, j, 0), block(k, j, 0), s1s.at[k, 3 - j], s1r.at[k, 3 - j], core, e).wait_recv()
                relay(k, (3 - j) // 2).start()
            remote(info(k, j, 0), info(k, j, 0), m1s.at[k, 3 - j], m1r.at[k, 3 - j], core, e).wait_recv()
            second_all(k, j)

    @pl.loop(0, RING)
    def _(t):
        j = gray(t)
        for k in range(3):
            for way in range(2):
                came = block(k, j, 3 - 2 * way)
                remote(came, came, s2s.at[k, j, way], s2r.at[k, j, way], core, e).wait_recv()
                third(k, j, way).start()
            for delta in (1, 3):
                came = info(k, j, 4 - delta)
                remote(came, came, m2s.at[k, j, delta - 1], m2r.at[k, j, delta - 1], core, e).wait_recv()

        @pl.loop(0, 3)
        def _(d):
            for k in range(3):
                pick(k, t * 3 + d, j, d + d // 2)

    for k in range(3):
        for n in range(2):
            put(k, n, 0, 0).wait()

    def span(q):
        return pl.ds(half_slots * q, half_slots)

    def cube(q, o, k, p):
        return r.at[(q, o, *cube_at(k, p), slice(None), cols(k))]

    def rod(q, o, k, p, d1):
        at = list(cube_at(k, p))
        at[dims(k)[1]] = d1
        return r.at[(q, o, *at, slice(None), cols(k))]

    def rod_out(q, k, p, d1, to):
        at = (d1, slice(None)) if k == 2 else (slice(None), d1)
        return s_ref.at[(p, to, *at, span(q), cols(k))]

    def early(k, j1, delta, to):
        i1, i2 = dims(k)[1:]
        d1 = lax.rem(v[i1] + j1, RING)
        return remote(rod_out(0, k, lax.rem(v[i2] + delta, RING), d1, to), rod(0, core, k, v[i2], d1), xes.at[k, j1, delta, to], xer.at[k, j1, delta, core], to, step(e, v[i2], st[i2], delta))

    def late(k, delta, to):
        i2 = dims(k)[2]
        return remote(s_ref.at[lax.rem(v[i2] + delta, RING), to, :, :, span(1), cols(k)], cube(1, core, k, v[i2]), xs.at[1, k, delta, to], xr.at[1, k, delta, core], to, step(e, v[i2], st[i2], delta))

    def beside(q, k):
        i2 = dims(k)[2]
        return remote(s_ref.at[v[i2], 1 - core, :, :, span(q), cols(k)], cube(q, core, k, v[i2]), xs.at[q, k, 0, 0], xr.at[q, k, 0, 0], 1 - core, e)

    def inward(q, k):
        i2 = dims(k)[2]
        return pltpu.make_async_copy(s_ref.at[v[i2], core, :, :, span(q), cols(k)], cube(q, core, k, v[i2]), loc.at[0, q, k])


    @pl.loop(0, 3)
    def _(d):
        for delta in DELTAS:
            for k in range(3):
                for to in range(2):
                    early(k, d + d // 2, delta, to).start()

    for load in loads:
        load.start()

    @pl.loop(0, RING)
    def _(t):
        j = gray(t)
        for k in range(3):
            for way in range(2):
                came = t2.at[(*at(k, j, 2), pl.ds(rows // 2 * way, rows // 2), cols(k))]
                remote(came, came, s3s.at[k, j, way], s3r.at[k, j, way], core, e).wait_recv()
            came = info(k, j, 2)
            remote(came, came, m2s.at[k, j, 1], m2r.at[k, j, 1], core, e).wait_recv()
            pick(k, t, j, 2)

    for k in range(3):
        for n in range(2):
            put(k, n, 0, 0).wait()
    for delta in DELTAS:
        for k in range(3):
            for to in range(2):
                early(k, 2, delta, to).start()
    for q in range(2):
        for k in range(3):
            beside(q, k).start()
            inward(q, k).start()
    for delta in DELTAS:
        for k in range(3):
            for to in range(2):
                late(k, delta, to).start()
    for load in loads:
        load.wait()

    def z4_at(q, k, p, c):
        return z4.at[q, p, c, :, :, :, cols(k)]

    def back(q, o, k, delta):
        i2 = dims(k)[2]
        here = views[o][i2]
        return remote(cube(q, o, k, lax.rem(here + delta, RING)), z4_at(q, k, here, core), s4.at[q, k, delta, o], r4.at[q, k, delta, core], o, step(e, here, STRIDES[o][i2], delta))

    def across(q, k):
        i2 = dims(k)[2]
        return remote(cube(q, 1 - core, k, other[i2]), z4_at(q, k, other[i2], core), s4.at[q, k, 0, 0], r4.at[q, k, 0, 0], 1 - core, e)

    def stay(q, k):
        i2 = dims(k)[2]
        return pltpu.make_async_copy(cube(q, core, k, v[i2]), z4_at(q, k, v[i2], core), loc.at[1, q, k])

    @pl.loop(0, 2)
    def _(q):
        for k in range(3):
            i1, i2 = dims(k)[1:]
            inward(q, k).wait()
            target = cube(q, 1 - core, k, other[i2])
            remote(target, target, xs.at[q, k, 0, 0], xr.at[q, k, 0, 0], core, e).wait_recv()

        @pl.when(q == 0)
        def _():
            @pl.loop(0, RING)
            def _(j1):
                for k in range(3):
                    i1, i2 = dims(k)[1:]
                    for delta in DELTAS:
                        for o in range(2):
                            target = rod(0, o, k, lax.rem(views[o][i2] + 4 - delta, RING), lax.rem(views[o][i1] + j1, RING))
                            remote(target, target, xes.at[k, j1, delta, 0], xer.at[k, j1, delta, o], core, e).wait_recv()

        @pl.when(q == 1)
        def _():
            for k in range(3):
                i2 = dims(k)[2]
                for delta in DELTAS:
                    for o in range(2):
                        target = cube(1, o, k, lax.rem(views[o][i2] + 4 - delta, RING))
                        remote(target, target, xs.at[1, k, delta, 0], xr.at[1, k, delta, o], core, e).wait_recv()

        for o in range(2):
            @pl.loop(0, RING)
            def _(i):
                x = r[q, o, i].reshape(RING * RING * half_slots, r.shape[-1])
                gate = jnp.dot(x, wg[...], preferred_element_type=jnp.float32)
                up = jnp.dot(x, wu[...], preferred_element_type=jnp.float32)
                hidden = (jax.nn.silu(gate) * up).astype(jnp.bfloat16)
                y = jnp.dot(hidden, wd[...], preferred_element_type=jnp.float32).astype(jnp.bfloat16)
                r[q, o, i] = y.reshape(RING, RING, half_slots, r.shape[-1])

            for delta in DELTAS:
                for k in range(3):
                    back(q, o, k, delta).start()
        for k in range(3):
            across(q, k).start()
            stay(q, k).start()

    def line(q, k, p):
        at = (slice(None), slice(None), p, slice(None)) if k == 2 else (slice(None), slice(None), slice(None), p)
        return z4.at[(q, *at, slice(None), cols(k))]

    def forth(q, k, delta):
        i1 = dims(k)[1]
        return remote(line(q, k, lax.rem(v[i1] + delta, RING)), z5.at[v[i1], :, :, :, span(q), cols(k)], s5.at[q, k, delta - 1], r5.at[q, k, delta - 1], core, step(e, v[i1], st[i1], delta))

    def lift(q, k, stage):
        i1 = dims(k)[1]
        room = bounce.at[q, :, :, :, :, cols(k)]
        if stage == 0:
            return pltpu.make_async_copy(line(q, k, v[i1]), room, loc.at[2, q, k])
        return pltpu.make_async_copy(room, z5.at[v[i1], :, :, :, span(q), cols(k)], loc.at[3, q, k])

    for q in range(2):
        for k in range(3):
            i2 = dims(k)[2]
            stay(q, k).wait()
            target = z4_at(q, k, v[i2], 1 - core)
            remote(target, target, s4.at[q, k, 0, 0], r4.at[q, k, 0, 0], core, e).wait_recv()
            for delta in DELTAS:
                for o in range(2):
                    target = z4_at(q, k, lax.rem(v[i2] + 4 - delta, RING), o)
                    remote(target, target, s4.at[q, k, delta, 0], r4.at[q, k, delta, o], core, e).wait_recv()
            for delta in DELTAS:
                forth(q, k, delta).start()
            lift(q, k, 0).start()
        for k in range(3):
            lift(q, k, 0).wait()
            lift(q, k, 1).start()
    @pl.loop(0, RING)
    def _(j):
        for k in range(3):
            for way in range(2):
                second(k, j, way).wait_send()
                third(k, j, way).wait_send()

    for k in range(3):
        for way in range(2):
            relay(k, way).wait_send()

    def fetch(q, turn, k, c):
        d0 = lax.rem(v[dims(k)[0]] + RING - turn + 2, RING)
        return pltpu.make_async_copy(z5.at[:, :, c, d0, span(q), cols(k)], t2.at[:, :, pl.ds(32 * (RING * q + turn) + half_slots * c, half_slots), cols(k)], load_sem.at[q, turn, k, c])

    def near(k, delta, part):
        i0 = dims(k)[0]
        at = pl.ds(rows // 2 * part, rows // 2)
        way = delta // 2
        return remote(sums.at[delta, at, cols(k)], came2.at[way, at, cols(k)], ps.at[k, way, part], pr.at[k, way, part], core, step(e, v[i0], st[i0], delta))

    def far(k, way):
        i0 = dims(k)[0]
        at = pl.ds(rows // 2 * way, rows // 2)
        return remote(sums.at[2, at, cols(k)], passing.at[way, :, cols(k)], hs.at[k, way], hr.at[k, way], core, step(e, v[i0], st[i0], 1 + 2 * way))

    def join(k, delta):
        way = delta // 2
        at = pl.ds(rows // 2 * way, rows // 2)
        remote(passing.at[way, :, cols(k)], passing.at[way, :, cols(k)], hs.at[k, way], hr.at[k, way], core, e).wait_recv()
        sums[delta, at, cols(k)] += passing[way, :, cols(k)]
        near(k, delta, way).start()

    n = RING * RING * 2 * half_slots
    lane = lax.broadcasted_iota(jnp.int32, (1, n), 1)
    place_of = (lane // (RING * 2 * half_slots), (lane // (2 * half_slots)) % RING, (lane // half_slots) % 2, lane % half_slots)

    def weigh(q, turn, delta, k):
        d1, p2, half, s = place_of
        i0, i1, i2 = dims(k)
        for c in range(2):
            fetch(q, turn, k, c).wait()
        a, b = at(k, delta, 0)
        m = jnp.transpose(mt[k, a, b])
        key = ((half * 64 + v[i0] * st[i0] + d1 * st[i1] + p2 * st[i2]) * slots + half_slots * q + s).astype(jnp.float32)
        w = jnp.zeros((rows, n), jnp.float32)
        for j in range(8):
            w = jnp.where(m[:, j:j + 1] == key, m[:, 8 + j:9 + j], w)
        hi = w.astype(jnp.bfloat16)
        rest = w - hi.astype(jnp.float32)
        mid = rest.astype(jnp.bfloat16)
        low = (rest - mid.astype(jnp.float32)).astype(jnp.bfloat16)
        y = t2[:, :, pl.ds(32 * (RING * q + turn), 32), cols(k)].reshape(n, COLS[k][1])
        total = jnp.dot(low, y, preferred_element_type=jnp.float32)
        total += jnp.dot(mid, y, preferred_element_type=jnp.float32)
        total += jnp.dot(hi, y, preferred_element_type=jnp.float32)
        if q == 0:
            sums[delta, :, cols(k)] = total
        else:
            sums[delta, :, cols(k)] += total

    def turn_delta(turn):
        return lax.rem(RING - turn + 2, RING)

    for q in range(2):
        for k in range(3):
            lift(q, k, 1).wait()
            i1 = dims(k)[1]
            for delta in DELTAS:
                target = z5.at[lax.rem(v[i1] + 4 - delta, RING), :, :, :, span(q), cols(k)]
                remote(target, target, s5.at[q, k, delta - 1], r5.at[q, k, delta - 1], core, e).wait_recv()
            for turn in range(RING):
                for c in range(2):
                    fetch(q, turn, k, c).start()

        @pl.loop(0, RING)
        def _(turn):
            for k in range(3):
                delta = turn_delta(turn)
                weigh(q, turn, delta, k)
                if q == 1:
                    @pl.when(turn == 0)
                    def _():
                        for way in range(2):
                            far(k, way).start()

                    @pl.when(turn == 1)
                    def _():
                        near(k, 1, 1).start()

                    @pl.when(turn == 3)
                    def _():
                        near(k, 3, 0).start()

            if q == 1:
                @pl.when(turn == 2)
                def _():
                    for k in range(3):
                        join(k, 1)

    for k in range(3):
        join(k, 3)
    keep = pltpu.make_async_copy(sums.at[0], own, load_sem.at[0, 0, 0, 0])
    keep.start()
    for k in range(3):
        for way in range(2):
            for part in range(2):
                target = came2.at[way, pl.ds(rows // 2 * part, rows // 2), cols(k)]
                remote(target, target, ps.at[k, way, part], pr.at[k, way, part], core, e).wait_recv()
    keep.wait()

    @pl.loop(0, RING)
    def _(j):
        for k in range(3):
            for delta in DELTAS:
                second_info(k, j, delta).wait_send()
                for to in range(2):
                    early(k, j, delta, to).wait_send()

    for k in range(3):
        for delta in DELTAS:
            if delta != 2:
                first(k, delta).wait_send()
            first_info(k, delta).wait_send()
            for to in range(2):
                late(k, delta, to).wait_send()

    for k in range(3):
        for way in range(2):
            far(k, way).wait_send()
            for part in range(2):
                near(k, 1 + 2 * way, part).wait_send()

    @pl.loop(0, 2)
    def _(q):
        for k in range(3):
            beside(q, k).wait_send()
            across(q, k).wait_send()
            for delta in DELTAS:
                forth(q, k, delta).wait_send()
                for o in range(2):
                    back(q, o, k, delta).wait_send()


def solution(mesh):
    group_axes = ("node", "expert")
    group_size = mesh.shape["node"] * mesh.shape["expert"]
    tok_spec = P(("data", "node", "expert"), None)
    weight_spec = P(("node", "expert"), None, None)
    hbm = pl.BlockSpec(memory_space=pltpu.HBM)
    vmem = pl.BlockSpec(memory_space=pltpu.VMEM)
    dma = pltpu.SemaphoreType.DMA

    def local_layer(tokens, expert_ids, gate_weights, slot_ids, w_gate, w_up, w_down):
        rows, width = tokens.shape
        top_k = expert_ids.shape[1]
        slots = capacity(rows, top_k, group_size)
        bf = jnp.bfloat16
        pos = jnp.where(slot_ids >= 0, expert_ids * slots + slot_ids, -1).astype(jnp.float32)
        meta = jnp.concatenate([pos.T, gate_weights.T], axis=0)
        f32 = jnp.float32
        own, came = pl.pallas_call(
            lambda *refs: layer_kernel(slots, *refs),
            name="layer",
            in_specs=[vmem, vmem, hbm, hbm, hbm],
            out_specs=[hbm] * 5,
            out_shape=[
                jax.ShapeDtypeStruct((4, 2, 4, 4, slots, width), bf), jax.ShapeDtypeStruct((2, 4, 2, 4, 4, slots // 2, width), bf),
                jax.ShapeDtypeStruct((4, 4, 2, 4, slots, width), bf), jax.ShapeDtypeStruct((rows, width), f32), jax.ShapeDtypeStruct((2, rows, width), f32),
            ],
            scratch_shapes=[pltpu.VMEM((3, 4, 4, 16, rows), f32), pltpu.VMEM((4, 4, rows, width), bf)] + [pltpu.VMEM((2, 4, 2, slots, n), bf) for _, n in COLS]
            + [pltpu.VMEM((2, 2, 4, 4, 4, slots // 2, width), bf), pltpu.VMEM((2, 4, 2, 4, slots // 2, width), bf)]
            + [pltpu.VMEM(w.shape[1:], bf) for w in (w_gate, w_up, w_down)]
            + [pltpu.VMEM((4, rows, width), f32), pltpu.VMEM((2, rows // 2, width), f32)]
            + [dma((2, 3)), dma((3, 2))] + [dma((3, 3))] * 4 + [dma((3, 4, 2))] * 2 + [dma((3, 4, 3))] * 2 + [dma((3, 4, 2))] * 2
            + [dma((3,)), dma((4, 2, 3))] + [dma((3, 4, 4, 2))] * 2 + [dma((2, 3, 4, 2))] * 4 + [dma((2, 3, 3))] * 2
            + [dma((3, 2))] * 2 + [dma((2, 4, 3, 2))] + [dma((3, 2))] * 2 + [dma((3, 2, 2))] * 2,
            compiler_params=pltpu.CompilerParams(collective_id=1, has_side_effects=True, vmem_limit_bytes=67043328),
        )(tokens, meta, w_gate, w_up, w_down)[3:]
        return (own + (came[0] + came[1])).astype(bf)

    return jax.shard_map(local_layer, mesh=mesh, in_specs=(tok_spec, tok_spec, tok_spec, tok_spec, weight_spec, weight_spec, weight_spec), out_specs=tok_spec, check_vma=False)
```

```python
import jax
import jax.numpy as jnp
from jax import lax
from jax.experimental import pallas as pl
from jax.experimental.pallas import tpu as pltpu
from jax.sharding import PartitionSpec as P

MESH = pl.DeviceIdType.MESH
CAP_FACTOR = 2
RING = 4
DELTAS = (1, 3, 2)
COLS = ((0, 768), (768, 640), (1408, 640))
STRIDES = ((16, 4, 1), (4, 1, 16))


def capacity(rows, top_k, experts):
    return ((CAP_FACTOR * rows * top_k + 8 * experts - 1) // (8 * experts)) * 8


def place():
    core, e = lax.axis_index("node"), lax.axis_index("expert")
    z, y, x = e // 16, (e // 4) % 4, e % 4
    return core, e, ((z, y, x), (y, x, z))


def own_view(core, views):
    v = tuple(a + core * (b - a) for a, b in zip(*views))
    s = tuple(a + core * (b - a) for a, b in zip(*STRIDES))
    return v, s


def step(e, pos, stride, delta):
    return e + (lax.rem(pos + delta, RING) - pos) * stride


def cols(k):
    return pl.ds(*COLS[k])


def dims(k):
    return k % 3, (k + 1) % 3, (k + 2) % 3


def plane_at(k, d0, d1):
    return (d1, d0) if k == 2 else (d0, d1)


def cube_at(k, p):
    full = [slice(None)] * 3
    full[dims(k)[2]] = p
    return tuple(full)


def remote(src, dst, send, recv, core, e):
    return pltpu.make_async_remote_copy(src_ref=src, dst_ref=dst, send_sem=send, recv_sem=recv, device_id=(0, core, e), device_id_type=MESH)


def greet(targets):
    barrier = pltpu.get_barrier_semaphore()
    for core, e in targets:
        pl.semaphore_signal(barrier, inc=1, device_id=(0, core, e), device_id_type=MESH)
    pl.semaphore_wait(barrier, len(targets))


def ring_peers(core_list, e, views):
    out = []
    for core in core_list:
        for v, s in zip(views[0], STRIDES[0]):
            for delta in DELTAS:
                out.append((core, step(e, v, s, delta)))
    return out


def layer_kernel(slots, tok, meta, wg_ref, wu_ref, wd_ref, s_ref, z4, z5, own, came2, mt, t2, tile0, tile1, tile2, r, bounce, wg, wu, wd, sums, passing,
                 loc0, out_sem, s1s, s1r, m1s, m1r, s2s, s2r, m2s, m2r, s3s, s3r, wsem, loc, xes, xer, xs, xr, s4, r4, s5, r5,
                 relay_s, relay_r, load_sem, hs, hr, ps, pr):
    core, e, views = place()
    v, st = own_view(core, views)
    other = own_view(1 - core, views)[0]
    half_slots = slots // 2
    loads = [pltpu.make_async_copy(src.at[0], dst, wsem.at[i]) for i, (src, dst) in enumerate(((wg_ref, wg), (wu_ref, wu), (wd_ref, wd)))]
    greet(ring_peers((0, 1), e, views) + [(1 - core, e)])
    rows = tok.shape[0]
    tiles = (tile0, tile1, tile2)

    def at(k, j0, j1):
        i0, i1, _ = dims(k)
        return plane_at(k, lax.rem(v[i0] + j0, RING), lax.rem(v[i1] + j1, RING))

    def block(k, j0, j1):
        return t2.at[(*at(k, j0, j1), slice(None), cols(k))]

    def info(k, j0, j1):
        return mt.at[(k, *at(k, j0, j1))]

    def first(k, delta):
        i0 = dims(k)[0]
        return remote(tok.at[:, cols(k)], block(k, 0, 0), s1s.at[k, delta - 1], s1r.at[k, delta - 1], core, step(e, v[i0], st[i0], delta))

    def first_info(k, delta):
        i0 = dims(k)[0]
        return remote(meta, info(k, 0, 0), m1s.at[k, delta - 1], m1r.at[k, delta - 1], core, step(e, v[i0], st[i0], delta))

    def relay(k, way):
        i0 = dims(k)[0]
        piece = t2.at[(*at(k, 3 - 2 * way, 0), pl.ds(rows // 2 * way, rows // 2), cols(k))]
        return remote(piece, piece, relay_s.at[k, way], relay_r.at[k, way], core, step(e, v[i0], st[i0], 1 + 2 * way))

    def second(k, j, way):
        i1 = dims(k)[1]
        return remote(block(k, j, 0), block(k, j, 0), s2s.at[k, j, way], s2r.at[k, j, way], core, step(e, v[i1], st[i1], 1 + 2 * way))

    def second_info(k, j, delta):
        i1 = dims(k)[1]
        return remote(info(k, j, 0), info(k, j, 0), m2s.at[k, j, delta - 1], m2r.at[k, j, delta - 1], core, step(e, v[i1], st[i1], delta))

    def third(k, j, way):
        i1 = dims(k)[1]
        piece = t2.at[(*at(k, j, 3 - 2 * way), pl.ds(rows // 2 * way, rows // 2), cols(k))]
        return remote(piece, piece, s3s.at[k, j, way], s3r.at[k, j, way], core, step(e, v[i1], st[i1], 1 + 2 * way))

    def second_all(k, j):
        for way in range(2):
            second(k, j, way).start()
        for delta in DELTAS:
            second_info(k, j, delta).start()

    def keep(k):
        return pltpu.make_async_copy(tok.at[:, cols(k)], block(k, 0, 0), loc0.at[0, k]), pltpu.make_async_copy(meta, info(k, 0, 0), loc0.at[1, k])

    def put(k, n, j0, j1):
        return pltpu.make_async_copy(tiles[k].at[lax.rem(n, 2)], s_ref.at[(slice(None), slice(None), *at(k, j0, j1), slice(None), cols(k))], out_sem.at[k, lax.rem(n, 2)])

    def pick(k, n, j0, j1):
        i0, i1, i2 = dims(k)
        total = RING * 2 * slots
        r = lax.broadcasted_iota(jnp.int32, (total, 1), 0)
        p2, half, s = r // (2 * slots), (r // slots) % 2, r % slots
        key = ((half * 64 + v[i0] * st[i0] + v[i1] * st[i1] + p2 * st[i2]) * slots + s).astype(jnp.float32)
        a, b = at(k, j0, j1)
        hot = jnp.zeros((total, rows), jnp.float32)
        for j in range(8):
            hot = jnp.where(key == mt[k, a, b, j:j + 1, :], 1.0, hot)
        got = jnp.dot(hot.astype(jnp.bfloat16), t2[a, b, :, cols(k)], preferred_element_type=jnp.float32)

        @pl.when(n >= 2)
        def _():
            put(k, n, j0, j1).wait()

        tiles[k][lax.rem(n, 2)] = got.astype(jnp.bfloat16).reshape(RING, 2, slots, COLS[k][1])
        put(k, n, j0, j1).start()

    def gray(t):
        return t + (t // 2) * (5 - 2 * t)

    for k in range(3):
        for copy in keep(k):
            copy.start()
    for delta in DELTAS:
        for k in range(3):
            if delta != 2:
                first(k, delta).start()
            first_info(k, delta).start()
    for k in range(3):
        for copy in keep(k):
            copy.wait()
        second_all(k, 0)
    for j in DELTAS:
        for k in range(3):
            if j == 2:
                for way in range(2):
                    piece = t2.at[(*at(k, 2, 0), pl.ds(rows // 2 * way, rows // 2), cols(k))]
                    remote(piece, piece, relay_s.at[k, way], relay_r.at[k, way], core, e).wait_recv()
            else:
                remote(block(k, j, 0), block(k, j, 0), s1s.at[k, 3 - j], s1r.at[k, 3 - j], core, e).wait_recv()
                relay(k, (3 - j) // 2).start()
            remote(info(k, j, 0), info(k, j, 0), m1s.at[k, 3 - j], m1r.at[k, 3 - j], core, e).wait_recv()
            second_all(k, j)

    @pl.loop(0, RING)
    def _(t):
        j = gray(t)
        for k in range(3):
            for way in range(2):
                came = block(k, j, 3 - 2 * way)
                remote(came, came, s2s.at[k, j, way], s2r.at[k, j, way], core, e).wait_recv()
                third(k, j, way).start()
            for delta in (1, 3):
                came = info(k, j, 4 - delta)
                remote(came, came, m2s.at[k, j, delta - 1], m2r.at[k, j, delta - 1], core, e).wait_recv()

        @pl.loop(0, 3)
        def _(d):
            for k in range(3):
                pick(k, t * 3 + d, j, d + d // 2)

    for k in range(3):
        for n in range(2):
            put(k, n, 0, 0).wait()

    def span(q):
        return pl.ds(half_slots * q, half_slots)

    def cube(q, o, k, p):
        return r.at[(q, o, *cube_at(k, p), slice(None), cols(k))]

    def rod(q, o, k, p, d1):
        at = list(cube_at(k, p))
        at[dims(k)[1]] = d1
        return r.at[(q, o, *at, slice(None), cols(k))]

    def rod_out(q, k, p, d1, to):
        at = (d1, slice(None)) if k == 2 else (slice(None), d1)
        return s_ref.at[(p, to, *at, span(q), cols(k))]

    def early(k, j1, delta, to):
        i1, i2 = dims(k)[1:]
        d1 = lax.rem(v[i1] + j1, RING)
        return remote(rod_out(0, k, lax.rem(v[i2] + delta, RING), d1, to), rod(0, core, k, v[i2], d1), xes.at[k, j1, delta, to], xer.at[k, j1, delta, core], to, step(e, v[i2], st[i2], delta))

    def late(k, delta, to):
        i2 = dims(k)[2]
        return remote(s_ref.at[lax.rem(v[i2] + delta, RING), to, :, :, span(1), cols(k)], cube(1, core, k, v[i2]), xs.at[1, k, delta, to], xr.at[1, k, delta, core], to, step(e, v[i2], st[i2], delta))

    def beside(q, k):
        i2 = dims(k)[2]
        return remote(s_ref.at[v[i2], 1 - core, :, :, span(q), cols(k)], cube(q, core, k, v[i2]), xs.at[q, k, 0, 0], xr.at[q, k, 0, 0], 1 - core, e)

    def inward(q, k):
        i2 = dims(k)[2]
        return pltpu.make_async_copy(s_ref.at[v[i2], core, :, :, span(q), cols(k)], cube(q, core, k, v[i2]), loc.at[0, q, k])


    @pl.loop(0, 3)
    def _(d):
        for delta in DELTAS:
            for k in range(3):
                for to in range(2):
                    early(k, d + d // 2, delta, to).start()

    for load in loads:
        load.start()

    @pl.loop(0, RING)
    def _(t):
        j = gray(t)
        for k in range(3):
            for way in range(2):
                came = t2.at[(*at(k, j, 2), pl.ds(rows // 2 * way, rows // 2), cols(k))]
                remote(came, came, s3s.at[k, j, way], s3r.at[k, j, way], core, e).wait_recv()
            came = info(k, j, 2)
            remote(came, came, m2s.at[k, j, 1], m2r.at[k, j, 1], core, e).wait_recv()
            pick(k, t, j, 2)

    for k in range(3):
        for n in range(2):
            put(k, n, 0, 0).wait()
    for delta in DELTAS:
        for k in range(3):
            for to in range(2):
                early(k, 2, delta, to).start()
    for q in range(2):
        for k in range(3):
            beside(q, k).start()
            inward(q, k).start()
    for delta in DELTAS:
        for k in range(3):
            for to in range(2):
                late(k, delta, to).start()
    for load in loads:
        load.wait()

    def z4_at(q, k, p, c):
        return z4.at[q, p, c, :, :, :, cols(k)]

    def back(q, o, k, delta):
        i2 = dims(k)[2]
        here = views[o][i2]
        return remote(cube(q, o, k, lax.rem(here + delta, RING)), z4_at(q, k, here, core), s4.at[q, k, delta, o], r4.at[q, k, delta, core], o, step(e, here, STRIDES[o][i2], delta))

    def across(q, k):
        i2 = dims(k)[2]
        return remote(cube(q, 1 - core, k, other[i2]), z4_at(q, k, other[i2], core), s4.at[q, k, 0, 0], r4.at[q, k, 0, 0], 1 - core, e)

    def stay(q, k):
        i2 = dims(k)[2]
        return pltpu.make_async_copy(cube(q, core, k, v[i2]), z4_at(q, k, v[i2], core), loc.at[1, q, k])

    @pl.loop(0, 2)
    def _(q):
        for k in range(3):
            i1, i2 = dims(k)[1:]
            inward(q, k).wait()
            target = cube(q, 1 - core, k, other[i2])
            remote(target, target, xs.at[q, k, 0, 0], xr.at[q, k, 0, 0], core, e).wait_recv()

        @pl.when(q == 0)
        def _():
            @pl.loop(0, RING)
            def _(j1):
                for k in range(3):
                    i1, i2 = dims(k)[1:]
                    for delta in DELTAS:
                        for o in range(2):
                            target = rod(0, o, k, lax.rem(views[o][i2] + 4 - delta, RING), lax.rem(views[o][i1] + j1, RING))
                            remote(target, target, xes.at[k, j1, delta, 0], xer.at[k, j1, delta, o], core, e).wait_recv()

        @pl.when(q == 1)
        def _():
            for k in range(3):
                i2 = dims(k)[2]
                for delta in DELTAS:
                    for o in range(2):
                        target = cube(1, o, k, lax.rem(views[o][i2] + 4 - delta, RING))
                        remote(target, target, xs.at[1, k, delta, 0], xr.at[1, k, delta, o], core, e).wait_recv()

        for o in range(2):
            @pl.loop(0, RING)
            def _(i):
                x = r[q, o, i].reshape(RING * RING * half_slots, r.shape[-1])
                gate = jnp.dot(x, wg[...], preferred_element_type=jnp.float32)
                up = jnp.dot(x, wu[...], preferred_element_type=jnp.float32)
                hidden = (jax.nn.silu(gate) * up).astype(jnp.bfloat16)
                y = jnp.dot(hidden, wd[...], preferred_element_type=jnp.float32).astype(jnp.bfloat16)
                r[q, o, i] = y.reshape(RING, RING, half_slots, r.shape[-1])

            for delta in DELTAS:
                for k in range(3):
                    back(q, o, k, delta).start()
        for k in range(3):
            across(q, k).start()
            stay(q, k).start()

    def line(q, k, p):
        at = (slice(None), slice(None), p, slice(None)) if k == 2 else (slice(None), slice(None), slice(None), p)
        return z4.at[(q, *at, slice(None), cols(k))]

    def forth(q, k, delta):
        i1 = dims(k)[1]
        return remote(line(q, k, lax.rem(v[i1] + delta, RING)), z5.at[v[i1], :, :, :, span(q), cols(k)], s5.at[q, k, delta - 1], r5.at[q, k, delta - 1], core, step(e, v[i1], st[i1], delta))

    def lift(q, k, stage):
        i1 = dims(k)[1]
        room = bounce.at[q, :, :, :, :, cols(k)]
        if stage == 0:
            return pltpu.make_async_copy(line(q, k, v[i1]), room, loc.at[2, q, k])
        return pltpu.make_async_copy(room, z5.at[v[i1], :, :, :, span(q), cols(k)], loc.at[3, q, k])

    for q in range(2):
        for k in range(3):
            i2 = dims(k)[2]
            stay(q, k).wait()
            target = z4_at(q, k, v[i2], 1 - core)
            remote(target, target, s4.at[q, k, 0, 0], r4.at[q, k, 0, 0], core, e).wait_recv()
            for delta in DELTAS:
                for o in range(2):
                    target = z4_at(q, k, lax.rem(v[i2] + 4 - delta, RING), o)
                    remote(target, target, s4.at[q, k, delta, 0], r4.at[q, k, delta, o], core, e).wait_recv()
            for delta in DELTAS:
                forth(q, k, delta).start()
            lift(q, k, 0).start()
        for k in range(3):
            lift(q, k, 0).wait()
            lift(q, k, 1).start()
    @pl.loop(0, RING)
    def _(j):
        for k in range(3):
            for way in range(2):
                second(k, j, way).wait_send()
                third(k, j, way).wait_send()

    for k in range(3):
        for way in range(2):
            relay(k, way).wait_send()

    @pl.loop(0, 2)
    def _(q):
        for k in range(3):
            across(q, k).wait_send()
            for delta in DELTAS:
                for o in range(2):
                    back(q, o, k, delta).wait_send()

    def fetch(q, turn, k, c):
        d0 = lax.rem(v[dims(k)[0]] + turn_delta(turn), RING)
        return pltpu.make_async_copy(z5.at[:, :, c, d0, span(q), cols(k)], t2.at[:, :, pl.ds(32 * (RING * q + turn) + half_slots * c, half_slots), cols(k)], load_sem.at[q, turn, k, c])

    def near(k, delta, part):
        i0 = dims(k)[0]
        at = pl.ds(rows // 2 * part, rows // 2)
        way = delta // 2
        return remote(sums.at[delta, at, cols(k)], came2.at[way, at, cols(k)], ps.at[k, way, part], pr.at[k, way, part], core, step(e, v[i0], st[i0], delta))

    def far(k, way):
        i0 = dims(k)[0]
        at = pl.ds(rows // 2 * way, rows // 2)
        return remote(sums.at[2, at, cols(k)], passing.at[way, :, cols(k)], hs.at[k, way], hr.at[k, way], core, step(e, v[i0], st[i0], 1 + 2 * way))

    def join(k, delta):
        way = delta // 2
        at = pl.ds(rows // 2 * way, rows // 2)
        remote(passing.at[way, :, cols(k)], passing.at[way, :, cols(k)], hs.at[k, way], hr.at[k, way], core, e).wait_recv()
        sums[delta, at, cols(k)] += passing[way, :, cols(k)]
        near(k, delta, way).start()

    n = RING * RING * 2 * half_slots
    lane = lax.broadcasted_iota(jnp.int32, (1, n), 1)
    place_of = (lane // (RING * 2 * half_slots), (lane // (2 * half_slots)) % RING, (lane // half_slots) % 2, lane % half_slots)

    def turn_delta(turn):
        h = turn // 2
        return (1 - h) * (2 - turn) + h * (9 - 3 * turn)

    def weights(q, delta, k):
        d1, p2, half, s = place_of
        i0, i1, i2 = dims(k)
        a, b = at(k, delta, 0)
        m = jnp.transpose(mt[k, a, b])
        key = ((half * 64 + v[i0] * st[i0] + d1 * st[i1] + p2 * st[i2]) * slots + half_slots * q + s).astype(jnp.float32)
        w = jnp.zeros((rows, n), jnp.float32)
        for j in range(8):
            w = jnp.where(m[:, j:j + 1] == key, m[:, 8 + j:9 + j], w)
        hi = w.astype(jnp.bfloat16)
        rest = w - hi.astype(jnp.float32)
        mid = rest.astype(jnp.bfloat16)
        low = (rest - mid.astype(jnp.float32)).astype(jnp.bfloat16)
        return low, mid, hi

    def weigh(q, turn, k, terms):
        for c in range(2):
            fetch(q, turn, k, c).wait()
        y = t2[:, :, pl.ds(32 * (RING * q + turn), 32), cols(k)].reshape(n, COLS[k][1])
        got = jnp.dot(jnp.concatenate(terms, axis=0), y, preferred_element_type=jnp.float32)
        return (got[:rows] + got[rows:2 * rows]) + got[2 * rows:]

    @pl.loop(0, RING)
    def _(turn):
        for k in range(3):
            for i, term in enumerate(weights(1, turn_delta(turn), k)):
                r[k // 2, k % 2, turn, :, :, :, pl.ds(n * i, n)] = term.reshape(RING, RING, half_slots, n)

    for q in range(2):
        for k in range(3):
            i1 = dims(k)[1]
            for delta in DELTAS:
                target = z5.at[lax.rem(v[i1] + 4 - delta, RING), :, :, :, span(q), cols(k)]
                remote(target, target, s5.at[q, k, delta - 1], r5.at[q, k, delta - 1], core, e).wait_recv()
            lift(q, k, 1).wait()
            for turn in range(RING):
                for c in range(2):
                    fetch(q, turn, k, c).start()

        @pl.loop(0, RING)
        def _(turn):
            delta = turn_delta(turn)
            for k in range(3):
                if q == 0:
                    sums[delta, :, cols(k)] = weigh(q, turn, k, weights(q, delta, k))
                else:
                    terms = [r[k // 2, k % 2, turn, :, :, :, pl.ds(n * i, n)].reshape(rows, n) for i in range(3)]
                    sums[delta, :, cols(k)] += weigh(q, turn, k, terms)

                    @pl.when(turn == 0)
                    def _():
                        for way in range(2):
                            far(k, way).start()

                    @pl.when(turn == 1)
                    def _():
                        near(k, 1, 1).start()

                    @pl.when(turn == 2)
                    def _():
                        near(k, 3, 0).start()

    for k in range(3):
        join(k, 1)
    for k in range(3):
        join(k, 3)
    keep = pltpu.make_async_copy(sums.at[0], own, load_sem.at[0, 0, 0, 0])
    keep.start()
    for k in range(3):
        for way in range(2):
            for part in range(2):
                target = came2.at[way, pl.ds(rows // 2 * part, rows // 2), cols(k)]
                remote(target, target, ps.at[k, way, part], pr.at[k, way, part], core, e).wait_recv()
    keep.wait()

    @pl.loop(0, RING)
    def _(j):
        for k in range(3):
            for delta in DELTAS:
                second_info(k, j, delta).wait_send()
                for to in range(2):
                    early(k, j, delta, to).wait_send()

    for k in range(3):
        for delta in DELTAS:
            if delta != 2:
                first(k, delta).wait_send()
            first_info(k, delta).wait_send()
            for to in range(2):
                late(k, delta, to).wait_send()

    for k in range(3):
        for way in range(2):
            far(k, way).wait_send()
            for part in range(2):
                near(k, 1 + 2 * way, part).wait_send()

    @pl.loop(0, 2)
    def _(q):
        for k in range(3):
            beside(q, k).wait_send()
            for delta in DELTAS:
                forth(q, k, delta).wait_send()


def solution(mesh):
    group_axes = ("node", "expert")
    group_size = mesh.shape["node"] * mesh.shape["expert"]
    tok_spec = P(("data", "node", "expert"), None)
    weight_spec = P(("node", "expert"), None, None)
    hbm = pl.BlockSpec(memory_space=pltpu.HBM)
    vmem = pl.BlockSpec(memory_space=pltpu.VMEM)
    dma = pltpu.SemaphoreType.DMA

    def local_layer(tokens, expert_ids, gate_weights, slot_ids, w_gate, w_up, w_down):
        rows, width = tokens.shape
        top_k = expert_ids.shape[1]
        slots = capacity(rows, top_k, group_size)
        bf = jnp.bfloat16
        pos = jnp.where(slot_ids >= 0, expert_ids * slots + slot_ids, -1).astype(jnp.float32)
        meta = jnp.concatenate([pos.T, gate_weights.T], axis=0)
        f32 = jnp.float32
        own, came = pl.pallas_call(
            lambda *refs: layer_kernel(slots, *refs),
            name="layer",
            in_specs=[vmem, vmem, hbm, hbm, hbm],
            out_specs=[hbm] * 5,
            out_shape=[
                jax.ShapeDtypeStruct((4, 2, 4, 4, slots, width), bf), jax.ShapeDtypeStruct((2, 4, 2, 4, 4, slots // 2, width), bf),
                jax.ShapeDtypeStruct((4, 4, 2, 4, slots, width), bf), jax.ShapeDtypeStruct((rows, width), f32), jax.ShapeDtypeStruct((2, rows, width), f32),
            ],
            scratch_shapes=[pltpu.VMEM((3, 4, 4, 16, rows), f32), pltpu.VMEM((4, 4, rows, width), bf)] + [pltpu.VMEM((2, 4, 2, slots, n), bf) for _, n in COLS]
            + [pltpu.VMEM((2, 2, 4, 4, 4, slots // 2, width), bf), pltpu.VMEM((2, 4, 2, 4, slots // 2, width), bf)]
            + [pltpu.VMEM(w.shape[1:], bf) for w in (w_gate, w_up, w_down)]
            + [pltpu.VMEM((4, rows, width), f32), pltpu.VMEM((2, rows // 2, width), f32)]
            + [dma((2, 3)), dma((3, 2))] + [dma((3, 3))] * 4 + [dma((3, 4, 2))] * 2 + [dma((3, 4, 3))] * 2 + [dma((3, 4, 2))] * 2
            + [dma((3,)), dma((4, 2, 3))] + [dma((3, 4, 4, 2))] * 2 + [dma((2, 3, 4, 2))] * 4 + [dma((2, 3, 3))] * 2
            + [dma((3, 2))] * 2 + [dma((2, 4, 3, 2))] + [dma((3, 2))] * 2 + [dma((3, 2, 2))] * 2,
            compiler_params=pltpu.CompilerParams(collective_id=1, has_side_effects=True, vmem_limit_bytes=67043328),
        )(tokens, meta, w_gate, w_up, w_down)[3:]
        return (own + (came[0] + came[1])).astype(bf)

    return jax.shard_map(local_layer, mesh=mesh, in_specs=(tok_spec, tok_spec, tok_spec, tok_spec, weight_spec, weight_spec, weight_spec), out_specs=tok_spec, check_vma=False)
```

```python
import jax
import jax.numpy as jnp
from jax import lax
from jax.experimental import pallas as pl
from jax.experimental.pallas import tpu as pltpu
from jax.sharding import PartitionSpec as P

MESH = pl.DeviceIdType.MESH
CAP_FACTOR = 2
RING = 4
DELTAS = (1, 3, 2)
COLS = ((0, 768), (768, 640), (1408, 640))
STRIDES = ((16, 4, 1), (4, 1, 16))


def capacity(rows, top_k, experts):
    return ((CAP_FACTOR * rows * top_k + 8 * experts - 1) // (8 * experts)) * 8


def place():
    core, e = lax.axis_index("node"), lax.axis_index("expert")
    z, y, x = e // 16, (e // 4) % 4, e % 4
    return core, e, ((z, y, x), (y, x, z))


def own_view(core, views):
    v = tuple(a + core * (b - a) for a, b in zip(*views))
    s = tuple(a + core * (b - a) for a, b in zip(*STRIDES))
    return v, s


def step(e, pos, stride, delta):
    return e + (lax.rem(pos + delta, RING) - pos) * stride


def cols(k):
    return pl.ds(*COLS[k])


def dims(k):
    return k % 3, (k + 1) % 3, (k + 2) % 3


def plane_at(k, d0, d1):
    return (d1, d0) if k == 2 else (d0, d1)


def cube_at(k, p):
    full = [slice(None)] * 3
    full[dims(k)[2]] = p
    return tuple(full)


def remote(src, dst, send, recv, core, e):
    return pltpu.make_async_remote_copy(src_ref=src, dst_ref=dst, send_sem=send, recv_sem=recv, device_id=(0, core, e), device_id_type=MESH)


def greet(targets):
    barrier = pltpu.get_barrier_semaphore()
    for core, e in targets:
        pl.semaphore_signal(barrier, inc=1, device_id=(0, core, e), device_id_type=MESH)
    pl.semaphore_wait(barrier, len(targets))


def ring_peers(core_list, e, views):
    out = []
    for core in core_list:
        for v, s in zip(views[0], STRIDES[0]):
            for delta in DELTAS:
                out.append((core, step(e, v, s, delta)))
    return out


def layer_kernel(slots, tok, where, gates, wg_ref, wu_ref, wd_ref, s_ref, z4, z5, own, came2, mt, t2, tile0, tile1, tile2, r, bounce, wg, wu, wd, sums, passing,
                 loc0, out_sem, s1s, s1r, m1s, m1r, s2s, s2r, m2s, m2r, s3s, s3r, wsem, loc, xes, xer, xs, xr, s4, r4, s5, r5,
                 relay_s, relay_r, load_sem, hs, hr, ps, pr, s6, r6, meta):
    core, e, views = place()
    v, st = own_view(core, views)
    other = own_view(1 - core, views)[0]
    half_slots = slots // 2
    loads = [pltpu.make_async_copy(src.at[0], dst, wsem.at[i]) for i, (src, dst) in enumerate(((wg_ref, wg), (wu_ref, wu), (wd_ref, wd)))]
    meta[:8] = where[...]
    meta[8:] = gates[...]
    greet(ring_peers((0, 1), e, views) + [(1 - core, e)])
    rows = tok.shape[0]
    tiles = (tile0, tile1, tile2)

    def at(k, j0, j1):
        i0, i1, _ = dims(k)
        return plane_at(k, lax.rem(v[i0] + j0, RING), lax.rem(v[i1] + j1, RING))

    def block(k, j0, j1):
        return t2.at[(*at(k, j0, j1), slice(None), cols(k))]

    def info(k, j0, j1):
        return mt.at[(k, *at(k, j0, j1))]

    def first(k, delta):
        i0 = dims(k)[0]
        return remote(tok.at[:, cols(k)], block(k, 0, 0), s1s.at[k, delta - 1], s1r.at[k, delta - 1], core, step(e, v[i0], st[i0], delta))

    def first_info(k, delta):
        i0 = dims(k)[0]
        return remote(meta, info(k, 0, 0), m1s.at[k, delta - 1], m1r.at[k, delta - 1], core, step(e, v[i0], st[i0], delta))

    def relay(k, way):
        i0 = dims(k)[0]
        piece = t2.at[(*at(k, 3 - 2 * way, 0), pl.ds(rows // 2 * way, rows // 2), cols(k))]
        return remote(piece, piece, relay_s.at[k, way], relay_r.at[k, way], core, step(e, v[i0], st[i0], 1 + 2 * way))

    def second(k, j, way):
        i1 = dims(k)[1]
        return remote(block(k, j, 0), block(k, j, 0), s2s.at[k, j, way], s2r.at[k, j, way], core, step(e, v[i1], st[i1], 1 + 2 * way))

    def second_info(k, j, delta):
        i1 = dims(k)[1]
        return remote(info(k, j, 0), info(k, j, 0), m2s.at[k, j, delta - 1], m2r.at[k, j, delta - 1], core, step(e, v[i1], st[i1], delta))

    def third(k, j, way):
        i1 = dims(k)[1]
        piece = t2.at[(*at(k, j, 3 - 2 * way), pl.ds(rows // 2 * way, rows // 2), cols(k))]
        return remote(piece, piece, s3s.at[k, j, way], s3r.at[k, j, way], core, step(e, v[i1], st[i1], 1 + 2 * way))

    def second_all(k, j):
        for way in range(2):
            second(k, j, way).start()
        for delta in DELTAS:
            second_info(k, j, delta).start()

    def keep(k):
        return pltpu.make_async_copy(tok.at[:, cols(k)], block(k, 0, 0), loc0.at[0, k]), pltpu.make_async_copy(meta, info(k, 0, 0), loc0.at[1, k])

    def put(k, n, j0, j1):
        return pltpu.make_async_copy(tiles[k].at[lax.rem(n, 2)], s_ref.at[(slice(None), slice(None), *at(k, j0, j1), slice(None), cols(k))], out_sem.at[k, lax.rem(n, 2)])

    def pick(k, n, j0, j1):
        i0, i1, i2 = dims(k)
        total = RING * 2 * slots
        r = lax.broadcasted_iota(jnp.int32, (total, 1), 0)
        p2, half, s = r // (2 * slots), (r // slots) % 2, r % slots
        key = ((half * 64 + v[i0] * st[i0] + v[i1] * st[i1] + p2 * st[i2]) * slots + s).astype(jnp.float32)
        a, b = at(k, j0, j1)
        hot = jnp.zeros((total, rows), jnp.float32)
        for j in range(8):
            hot = jnp.where(key == mt[k, a, b, j:j + 1, :], 1.0, hot)
        got = jnp.dot(hot.astype(jnp.bfloat16), t2[a, b, :, cols(k)], preferred_element_type=jnp.float32)

        @pl.when(n >= 2)
        def _():
            put(k, n, j0, j1).wait()

        tiles[k][lax.rem(n, 2)] = got.astype(jnp.bfloat16).reshape(RING, 2, slots, COLS[k][1])
        put(k, n, j0, j1).start()

    def gray(t):
        return t + (t // 2) * (5 - 2 * t)

    for k in range(3):
        for copy in keep(k):
            copy.start()
    for delta in DELTAS:
        for k in range(3):
            if delta != 2:
                first(k, delta).start()
            first_info(k, delta).start()
    for k in range(3):
        for copy in keep(k):
            copy.wait()
        second_all(k, 0)
    for j in DELTAS:
        for k in range(3):
            if j == 2:
                for way in range(2):
                    piece = t2.at[(*at(k, 2, 0), pl.ds(rows // 2 * way, rows // 2), cols(k))]
                    remote(piece, piece, relay_s.at[k, way], relay_r.at[k, way], core, e).wait_recv()
            else:
                remote(block(k, j, 0), block(k, j, 0), s1s.at[k, 3 - j], s1r.at[k, 3 - j], core, e).wait_recv()
                relay(k, (3 - j) // 2).start()
            remote(info(k, j, 0), info(k, j, 0), m1s.at[k, 3 - j], m1r.at[k, 3 - j], core, e).wait_recv()
            second_all(k, j)

    @pl.loop(0, RING)
    def _(t):
        j = gray(t)
        for k in range(3):
            for way in range(2):
                came = block(k, j, 3 - 2 * way)
                remote(came, came, s2s.at[k, j, way], s2r.at[k, j, way], core, e).wait_recv()
                third(k, j, way).start()
            for delta in (1, 3):
                came = info(k, j, 4 - delta)
                remote(came, came, m2s.at[k, j, delta - 1], m2r.at[k, j, delta - 1], core, e).wait_recv()

        @pl.loop(0, 3)
        def _(d):
            for k in range(3):
                pick(k, t * 3 + d, j, d + d // 2)

    for k in range(3):
        for n in range(2):
            put(k, n, 0, 0).wait()

    def span(q):
        return pl.ds(half_slots * q, half_slots)

    def cube(q, o, k, p):
        return r.at[(q, o, *cube_at(k, p), slice(None), cols(k))]

    def rod(q, o, k, p, d1):
        at = list(cube_at(k, p))
        at[dims(k)[1]] = d1
        return r.at[(q, o, *at, slice(None), cols(k))]

    def rod_out(q, k, p, d1, to):
        at = (d1, slice(None)) if k == 2 else (slice(None), d1)
        return s_ref.at[(p, to, *at, span(q), cols(k))]

    def early(k, j1, delta, to):
        i1, i2 = dims(k)[1:]
        d1 = lax.rem(v[i1] + j1, RING)
        return remote(rod_out(0, k, lax.rem(v[i2] + delta, RING), d1, to), rod(0, core, k, v[i2], d1), xes.at[k, j1, delta, to], xer.at[k, j1, delta, core], to, step(e, v[i2], st[i2], delta))

    def late(k, delta, to):
        i2 = dims(k)[2]
        return remote(s_ref.at[lax.rem(v[i2] + delta, RING), to, :, :, span(1), cols(k)], cube(1, core, k, v[i2]), xs.at[1, k, delta, to], xr.at[1, k, delta, core], to, step(e, v[i2], st[i2], delta))

    def beside(q, k):
        i2 = dims(k)[2]
        return remote(s_ref.at[v[i2], 1 - core, :, :, span(q), cols(k)], cube(q, core, k, v[i2]), xs.at[q, k, 0, 0], xr.at[q, k, 0, 0], 1 - core, e)

    def inward(q, k):
        i2 = dims(k)[2]
        return pltpu.make_async_copy(s_ref.at[v[i2], core, :, :, span(q), cols(k)], cube(q, core, k, v[i2]), loc.at[0, q, k])


    @pl.loop(0, 3)
    def _(d):
        for delta in DELTAS:
            for k in range(3):
                for to in range(2):
                    early(k, d + d // 2, delta, to).start()

    for load in loads:
        load.start()

    @pl.loop(0, RING)
    def _(t):
        j = gray(t)
        for k in range(3):
            for way in range(2):
                came = t2.at[(*at(k, j, 2), pl.ds(rows // 2 * way, rows // 2), cols(k))]
                remote(came, came, s3s.at[k, j, way], s3r.at[k, j, way], core, e).wait_recv()
            came = info(k, j, 2)
            remote(came, came, m2s.at[k, j, 1], m2r.at[k, j, 1], core, e).wait_recv()
            pick(k, t, j, 2)

    for k in range(3):
        for n in range(2):
            put(k, n, 0, 0).wait()
    for delta in DELTAS:
        for k in range(3):
            for to in range(2):
                early(k, 2, delta, to).start()
    for q in range(2):
        for k in range(3):
            beside(q, k).start()
            inward(q, k).start()
    for delta in DELTAS:
        for k in range(3):
            for to in range(2):
                late(k, delta, to).start()
    for load in loads:
        load.wait()

    def z4_at(q, k, p, c):
        return z4.at[q, p, c, :, :, :, cols(k)]

    def back(q, o, k, delta):
        i2 = dims(k)[2]
        here = views[o][i2]
        return remote(cube(q, o, k, lax.rem(here + delta, RING)), z4_at(q, k, here, core), s4.at[q, k, delta, o], r4.at[q, k, delta, core], o, step(e, here, STRIDES[o][i2], delta))

    def across(q, k):
        i2 = dims(k)[2]
        return remote(cube(q, 1 - core, k, other[i2]), z4_at(q, k, other[i2], core), s4.at[q, k, 0, 0], r4.at[q, k, 0, 0], 1 - core, e)

    def stay(q, k):
        i2 = dims(k)[2]
        return pltpu.make_async_copy(cube(q, core, k, v[i2]), z4_at(q, k, v[i2], core), loc.at[1, q, k])

    @pl.loop(0, 2)
    def _(q):
        for k in range(3):
            i1, i2 = dims(k)[1:]
            inward(q, k).wait()
            target = cube(q, 1 - core, k, other[i2])
            remote(target, target, xs.at[q, k, 0, 0], xr.at[q, k, 0, 0], core, e).wait_recv()

        @pl.when(q == 0)
        def _():
            @pl.loop(0, RING)
            def _(j1):
                for k in range(3):
                    i1, i2 = dims(k)[1:]
                    for delta in DELTAS:
                        for o in range(2):
                            target = rod(0, o, k, lax.rem(views[o][i2] + 4 - delta, RING), lax.rem(views[o][i1] + j1, RING))
                            remote(target, target, xes.at[k, j1, delta, 0], xer.at[k, j1, delta, o], core, e).wait_recv()

        @pl.when(q == 1)
        def _():
            for k in range(3):
                i2 = dims(k)[2]
                for delta in DELTAS:
                    for o in range(2):
                        target = cube(1, o, k, lax.rem(views[o][i2] + 4 - delta, RING))
                        remote(target, target, xs.at[1, k, delta, 0], xr.at[1, k, delta, o], core, e).wait_recv()

        for o in range(2):
            @pl.loop(0, RING)
            def _(i):
                x = r[q, o, i].reshape(RING * RING * half_slots, r.shape[-1])
                gate = jnp.dot(x, wg[...], preferred_element_type=jnp.float32)
                up = jnp.dot(x, wu[...], preferred_element_type=jnp.float32)
                hidden = (jax.nn.silu(gate) * up).astype(jnp.bfloat16)
                y = jnp.dot(hidden, wd[...], preferred_element_type=jnp.float32).astype(jnp.bfloat16)
                r[q, o, i] = y.reshape(RING, RING, half_slots, r.shape[-1])

            for delta in DELTAS:
                for k in range(3):
                    back(q, o, k, delta).start()
        for k in range(3):
            across(q, k).start()
            stay(q, k).start()

    def line(q, k, p):
        at = (slice(None), slice(None), p, slice(None)) if k == 2 else (slice(None), slice(None), slice(None), p)
        return z4.at[(q, *at, slice(None), cols(k))]

    def forth(q, k, delta):
        i1 = dims(k)[1]
        return remote(line(q, k, lax.rem(v[i1] + delta, RING)), z5.at[v[i1], :, :, :, span(q), cols(k)], s5.at[q, k, delta - 1], r5.at[q, k, delta - 1], core, step(e, v[i1], st[i1], delta))

    def turn_delta(turn):
        h = turn // 2
        return (1 - h) * (2 - turn) + h * (9 - 3 * turn)

    def column(turn, k, from_d1):
        d0 = lax.rem(v[dims(k)[0]] + turn_delta(turn), RING)
        return z5.at[from_d1, :, :, d0, span(1), cols(k)]

    def single(turn, k, delta):
        i0, i1, _ = dims(k)
        d0, d1 = lax.rem(v[i0] + turn_delta(turn), RING), lax.rem(v[i1] + delta, RING)
        src = z4.at[(1, slice(None), slice(None), *plane_at(k, d0, d1), slice(None), cols(k))]
        return remote(src, column(turn, k, v[i1]), s6.at[k, turn, delta - 1], r6.at[k, turn, delta - 1], core, step(e, v[i1], st[i1], delta))

    def lift(q, k, stage):
        i1 = dims(k)[1]
        room = bounce.at[q, :, :, :, :, cols(k)]
        if stage == 0:
            return pltpu.make_async_copy(line(q, k, v[i1]), room, loc.at[2, q, k])
        return pltpu.make_async_copy(room, z5.at[v[i1], :, :, :, span(q), cols(k)], loc.at[3, q, k])

    for q in range(2):
        for k in range(3):
            i2 = dims(k)[2]
            stay(q, k).wait()
            target = z4_at(q, k, v[i2], 1 - core)
            remote(target, target, s4.at[q, k, 0, 0], r4.at[q, k, 0, 0], core, e).wait_recv()
            for delta in DELTAS:
                for o in range(2):
                    target = z4_at(q, k, lax.rem(v[i2] + 4 - delta, RING), o)
                    remote(target, target, s4.at[q, k, delta, 0], r4.at[q, k, delta, o], core, e).wait_recv()
            if q == 0:
                for delta in DELTAS:
                    forth(q, k, delta).start()
            lift(q, k, 0).start()
        if q == 1:
            @pl.loop(0, RING)
            def _(turn):
                for k in range(3):
                    for delta in DELTAS:
                        single(turn, k, delta).start()

        for k in range(3):
            lift(q, k, 0).wait()
            lift(q, k, 1).start()
    @pl.loop(0, RING)
    def _(j):
        for k in range(3):
            for way in range(2):
                second(k, j, way).wait_send()
                third(k, j, way).wait_send()

    for k in range(3):
        for way in range(2):
            relay(k, way).wait_send()

    @pl.loop(0, 2)
    def _(q):
        for k in range(3):
            across(q, k).wait_send()
            for delta in DELTAS:
                for o in range(2):
                    back(q, o, k, delta).wait_send()

    def fetch(q, turn, k, c):
        d0 = lax.rem(v[dims(k)[0]] + turn_delta(turn), RING)
        return pltpu.make_async_copy(z5.at[:, :, c, d0, span(q), cols(k)], t2.at[:, :, pl.ds(32 * (RING * q + turn) + half_slots * c, half_slots), cols(k)], load_sem.at[q, turn, k, c])

    def near(k, delta, part):
        i0 = dims(k)[0]
        at = pl.ds(rows // 2 * part, rows // 2)
        way = delta // 2
        return remote(sums.at[delta, at, cols(k)], came2.at[way, at, cols(k)], ps.at[k, way, part], pr.at[k, way, part], core, step(e, v[i0], st[i0], delta))

    def far(k, way):
        i0 = dims(k)[0]
        at = pl.ds(rows // 2 * way, rows // 2)
        return remote(sums.at[2, at, cols(k)], passing.at[way, :, cols(k)], hs.at[k, way], hr.at[k, way], core, step(e, v[i0], st[i0], 1 + 2 * way))

    def join(k, delta):
        way = delta // 2
        at = pl.ds(rows // 2 * way, rows // 2)
        remote(passing.at[way, :, cols(k)], passing.at[way, :, cols(k)], hs.at[k, way], hr.at[k, way], core, e).wait_recv()
        sums[delta, at, cols(k)] += passing[way, :, cols(k)]
        near(k, delta, way).start()

    n = RING * RING * 2 * half_slots
    lane = lax.broadcasted_iota(jnp.int32, (1, n), 1)
    place_of = (lane // (RING * 2 * half_slots), (lane // (2 * half_slots)) % RING, (lane // half_slots) % 2, lane % half_slots)

    def weights(q, delta, k):
        d1, p2, half, s = place_of
        i0, i1, i2 = dims(k)
        a, b = at(k, delta, 0)
        m = jnp.transpose(mt[k, a, b])
        key = ((half * 64 + v[i0] * st[i0] + d1 * st[i1] + p2 * st[i2]) * slots + half_slots * q + s).astype(jnp.float32)
        w = jnp.zeros((rows, n), jnp.float32)
        for j in range(8):
            w = jnp.where(m[:, j:j + 1] == key, m[:, 8 + j:9 + j], w)
        hi = w.astype(jnp.bfloat16)
        rest = w - hi.astype(jnp.float32)
        mid = rest.astype(jnp.bfloat16)
        low = (rest - mid.astype(jnp.float32)).astype(jnp.bfloat16)
        return low, mid, hi

    def weigh(q, turn, k, terms):
        for c in range(2):
            fetch(q, turn, k, c).wait()
        y = t2[:, :, pl.ds(32 * (RING * q + turn), 32), cols(k)].reshape(n, COLS[k][1])
        got = jnp.dot(jnp.concatenate(terms, axis=0), y, preferred_element_type=jnp.float32)
        return (got[:rows] + got[rows:2 * rows]) + got[2 * rows:]

    @pl.loop(0, RING)
    def _(turn):
        for k in range(3):
            for i, term in enumerate(weights(1, turn_delta(turn), k)):
                r[k // 2, k % 2, turn, :, :, :, pl.ds(n * i, n)] = term.reshape(RING, RING, half_slots, n)

    for q in range(2):
        for k in range(3):
            lift(q, k, 1).wait()
        if q == 0:
            for k in range(3):
                i1 = dims(k)[1]
                for delta in DELTAS:
                    target = z5.at[lax.rem(v[i1] + 4 - delta, RING), :, :, :, span(0), cols(k)]
                    remote(target, target, s5.at[0, k, delta - 1], r5.at[0, k, delta - 1], core, e).wait_recv()
                for turn in range(RING):
                    for c in range(2):
                        fetch(0, turn, k, c).start()

        @pl.loop(0, RING)
        def _(turn):
            delta = turn_delta(turn)
            if q == 1:
                for k in range(3):
                    i1 = dims(k)[1]
                    for d in DELTAS:
                        target = column(turn, k, lax.rem(v[i1] + 4 - d, RING))
                        remote(target, target, s6.at[k, turn, d - 1], r6.at[k, turn, d - 1], core, e).wait_recv()
                    for c in range(2):
                        fetch(1, turn, k, c).start()
            for k in range(3):
                if q == 0:
                    sums[delta, :, cols(k)] = weigh(q, turn, k, weights(q, delta, k))
                else:
                    terms = [r[k // 2, k % 2, turn, :, :, :, pl.ds(n * i, n)].reshape(rows, n) for i in range(3)]
                    sums[delta, :, cols(k)] += weigh(q, turn, k, terms)

                    @pl.when(turn == 0)
                    def _():
                        for way in range(2):
                            far(k, way).start()

                    @pl.when(turn == 1)
                    def _():
                        near(k, 1, 1).start()

                    @pl.when(turn == 2)
                    def _():
                        near(k, 3, 0).start()

    for k in range(3):
        join(k, 1)
    for k in range(3):
        join(k, 3)
    keep = pltpu.make_async_copy(sums.at[0], own, load_sem.at[0, 0, 0, 0])
    keep.start()
    for k in range(3):
        for way in range(2):
            for part in range(2):
                target = came2.at[way, pl.ds(rows // 2 * part, rows // 2), cols(k)]
                remote(target, target, ps.at[k, way, part], pr.at[k, way, part], core, e).wait_recv()
    keep.wait()

    @pl.loop(0, RING)
    def _(j):
        for k in range(3):
            for delta in DELTAS:
                single(j, k, delta).wait_send()
                second_info(k, j, delta).wait_send()
                for to in range(2):
                    early(k, j, delta, to).wait_send()

    for k in range(3):
        for delta in DELTAS:
            if delta != 2:
                first(k, delta).wait_send()
            first_info(k, delta).wait_send()
            forth(0, k, delta).wait_send()
            for to in range(2):
                late(k, delta, to).wait_send()

    for k in range(3):
        for way in range(2):
            far(k, way).wait_send()
            for part in range(2):
                near(k, 1 + 2 * way, part).wait_send()

    @pl.loop(0, 2)
    def _(q):
        for k in range(3):
            beside(q, k).wait_send()


def solution(mesh):
    group_axes = ("node", "expert")
    group_size = mesh.shape["node"] * mesh.shape["expert"]
    tok_spec = P(("data", "node", "expert"), None)
    weight_spec = P(("node", "expert"), None, None)
    hbm = pl.BlockSpec(memory_space=pltpu.HBM)
    vmem = pl.BlockSpec(memory_space=pltpu.VMEM)
    dma = pltpu.SemaphoreType.DMA

    def local_layer(tokens, expert_ids, gate_weights, slot_ids, w_gate, w_up, w_down):
        rows, width = tokens.shape
        top_k = expert_ids.shape[1]
        slots = capacity(rows, top_k, group_size)
        bf = jnp.bfloat16
        pos = jnp.where(slot_ids >= 0, expert_ids * slots + slot_ids, -1).astype(jnp.float32)
        f32 = jnp.float32
        own, came = pl.pallas_call(
            lambda *refs: layer_kernel(slots, *refs),
            name="layer",
            in_specs=[vmem, vmem, vmem, hbm, hbm, hbm],
            out_specs=[hbm] * 5,
            out_shape=[
                jax.ShapeDtypeStruct((4, 2, 4, 4, slots, width), bf), jax.ShapeDtypeStruct((2, 4, 2, 4, 4, slots // 2, width), bf),
                jax.ShapeDtypeStruct((4, 4, 2, 4, slots, width), bf), jax.ShapeDtypeStruct((rows, width), f32), jax.ShapeDtypeStruct((2, rows, width), f32),
            ],
            scratch_shapes=[pltpu.VMEM((3, 4, 4, 16, rows), f32), pltpu.VMEM((4, 4, rows, width), bf)] + [pltpu.VMEM((2, 4, 2, slots, n), bf) for _, n in COLS]
            + [pltpu.VMEM((2, 2, 4, 4, 4, slots // 2, width), bf), pltpu.VMEM((2, 4, 2, 4, slots // 2, width), bf)]
            + [pltpu.VMEM(w.shape[1:], bf) for w in (w_gate, w_up, w_down)]
            + [pltpu.VMEM((4, rows, width), f32), pltpu.VMEM((2, rows // 2, width), f32)]
            + [dma((2, 3)), dma((3, 2))] + [dma((3, 3))] * 4 + [dma((3, 4, 2))] * 2 + [dma((3, 4, 3))] * 2 + [dma((3, 4, 2))] * 2
            + [dma((3,)), dma((4, 2, 3))] + [dma((3, 4, 4, 2))] * 2 + [dma((2, 3, 4, 2))] * 4 + [dma((2, 3, 3))] * 2
            + [dma((3, 2))] * 2 + [dma((2, 4, 3, 2))] + [dma((3, 2))] * 2 + [dma((3, 2, 2))] * 2
            + [dma((3, 4, 3))] * 2 + [pltpu.VMEM((16, rows), f32)],
            compiler_params=pltpu.CompilerParams(collective_id=1, has_side_effects=True, vmem_limit_bytes=67043328),
        )(tokens, pos.T, gate_weights.T, w_gate, w_up, w_down)[3:]
        return (own + (came[0] + came[1])).astype(bf)

    return jax.shard_map(local_layer, mesh=mesh, in_specs=(tok_spec, tok_spec, tok_spec, tok_spec, weight_spec, weight_spec, weight_spec), out_specs=tok_spec, check_vma=False)
```

```python
import jax
import jax.numpy as jnp
from jax import lax
from jax.experimental import pallas as pl
from jax.experimental.pallas import tpu as pltpu
from jax.sharding import PartitionSpec as P

MESH = pl.DeviceIdType.MESH
CAP_FACTOR = 2
RING = 4
DELTAS = (1, 3, 2)
COLS = ((0, 768), (768, 640), (1408, 640))
STRIDES = ((16, 4, 1), (4, 1, 16))


def capacity(rows, top_k, experts):
    return ((CAP_FACTOR * rows * top_k + 8 * experts - 1) // (8 * experts)) * 8


def place():
    core, e = lax.axis_index("node"), lax.axis_index("expert")
    z, y, x = e // 16, (e // 4) % 4, e % 4
    return core, e, ((z, y, x), (y, x, z))


def own_view(core, views):
    v = tuple(a + core * (b - a) for a, b in zip(*views))
    s = tuple(a + core * (b - a) for a, b in zip(*STRIDES))
    return v, s


def step(e, pos, stride, delta):
    return e + (lax.rem(pos + delta, RING) - pos) * stride


def cols(k):
    return pl.ds(*COLS[k])


def dims(k):
    return k % 3, (k + 1) % 3, (k + 2) % 3


def plane_at(k, d0, d1):
    return (d1, d0) if k == 2 else (d0, d1)


def cube_at(k, p):
    full = [slice(None)] * 3
    full[dims(k)[2]] = p
    return tuple(full)


def remote(src, dst, send, recv, core, e):
    return pltpu.make_async_remote_copy(src_ref=src, dst_ref=dst, send_sem=send, recv_sem=recv, device_id=(0, core, e), device_id_type=MESH)


def greet(targets):
    barrier = pltpu.get_barrier_semaphore()
    for core, e in targets:
        pl.semaphore_signal(barrier, inc=1, device_id=(0, core, e), device_id_type=MESH)
    pl.semaphore_wait(barrier, len(targets))


def ring_peers(core_list, e, views):
    out = []
    for core in core_list:
        for v, s in zip(views[0], STRIDES[0]):
            for delta in DELTAS:
                out.append((core, step(e, v, s, delta)))
    return out


def layer_kernel(slots, tok, ids, slot_of, gates, wg_ref, wu_ref, wd_ref, s_ref, z4, z5, own, came2, mt, t2, tile0, tile1, tile2, r, bounce, wg, wu, wd, sums, passing,
                 loc0, out_sem, s1s, s1r, m1s, m1r, s2s, s2r, m2s, m2r, s3s, s3r, wsem, loc, xes, xer, xs, xr, s4, r4, s5, r5,
                 relay_s, relay_r, load_sem, hs, hr, ps, pr, s6, r6, meta):
    core, e, views = place()
    v, st = own_view(core, views)
    other = own_view(1 - core, views)[0]
    half_slots = slots // 2
    loads = [pltpu.make_async_copy(src.at[0], dst, wsem.at[i]) for i, (src, dst) in enumerate(((wg_ref, wg), (wu_ref, wu), (wd_ref, wd)))]
    meta[:8] = jnp.where(slot_of[...] >= 0, ids[...] * slots + slot_of[...], -1).astype(jnp.float32)
    meta[8:] = gates[...]
    greet(ring_peers((0, 1), e, views) + [(1 - core, e)])
    rows = tok.shape[0]
    tiles = (tile0, tile1, tile2)

    def at(k, j0, j1):
        i0, i1, _ = dims(k)
        return plane_at(k, lax.rem(v[i0] + j0, RING), lax.rem(v[i1] + j1, RING))

    def block(k, j0, j1):
        return t2.at[(*at(k, j0, j1), slice(None), cols(k))]

    def info(k, j0, j1):
        return mt.at[(k, *at(k, j0, j1))]

    def first(k, delta):
        i0 = dims(k)[0]
        return remote(tok.at[:, cols(k)], block(k, 0, 0), s1s.at[k, delta - 1], s1r.at[k, delta - 1], core, step(e, v[i0], st[i0], delta))

    def first_info(k, delta):
        i0 = dims(k)[0]
        return remote(meta, info(k, 0, 0), m1s.at[k, delta - 1], m1r.at[k, delta - 1], core, step(e, v[i0], st[i0], delta))

    def relay(k, way):
        i0 = dims(k)[0]
        piece = t2.at[(*at(k, 3 - 2 * way, 0), pl.ds(rows // 2 * way, rows // 2), cols(k))]
        return remote(piece, piece, relay_s.at[k, way], relay_r.at[k, way], core, step(e, v[i0], st[i0], 1 + 2 * way))

    def second(k, j, way):
        i1 = dims(k)[1]
        return remote(block(k, j, 0), block(k, j, 0), s2s.at[k, j, way], s2r.at[k, j, way], core, step(e, v[i1], st[i1], 1 + 2 * way))

    def second_info(k, j, delta):
        i1 = dims(k)[1]
        return remote(info(k, j, 0), info(k, j, 0), m2s.at[k, j, delta - 1], m2r.at[k, j, delta - 1], core, step(e, v[i1], st[i1], delta))

    def third(k, j, way):
        i1 = dims(k)[1]
        piece = t2.at[(*at(k, j, 3 - 2 * way), pl.ds(rows // 2 * way, rows // 2), cols(k))]
        return remote(piece, piece, s3s.at[k, j, way], s3r.at[k, j, way], core, step(e, v[i1], st[i1], 1 + 2 * way))

    def second_all(k, j):
        for way in range(2):
            second(k, j, way).start()
        for delta in DELTAS:
            second_info(k, j, delta).start()

    def keep(k):
        return pltpu.make_async_copy(tok.at[:, cols(k)], block(k, 0, 0), loc0.at[0, k]), pltpu.make_async_copy(meta, info(k, 0, 0), loc0.at[1, k])

    def put(k, n, j0, j1):
        return pltpu.make_async_copy(tiles[k].at[lax.rem(n, 2)], s_ref.at[(slice(None), slice(None), *at(k, j0, j1), slice(None), cols(k))], out_sem.at[k, lax.rem(n, 2)])

    def pick(k, n, j0, j1):
        i0, i1, i2 = dims(k)
        total = RING * 2 * slots
        r = lax.broadcasted_iota(jnp.int32, (total, 1), 0)
        p2, half, s = r // (2 * slots), (r // slots) % 2, r % slots
        key = ((half * 64 + v[i0] * st[i0] + v[i1] * st[i1] + p2 * st[i2]) * slots + s).astype(jnp.float32)
        a, b = at(k, j0, j1)
        hot = jnp.zeros((total, rows), jnp.float32)
        for j in range(8):
            hot = jnp.where(key == mt[k, a, b, j:j + 1, :], 1.0, hot)
        got = jnp.dot(hot.astype(jnp.bfloat16), t2[a, b, :, cols(k)], preferred_element_type=jnp.float32)

        @pl.when(n >= 2)
        def _():
            put(k, n, j0, j1).wait()

        tiles[k][lax.rem(n, 2)] = got.astype(jnp.bfloat16).reshape(RING, 2, slots, COLS[k][1])
        put(k, n, j0, j1).start()

    def gray(t):
        return t + (t // 2) * (5 - 2 * t)

    for k in range(3):
        for copy in keep(k):
            copy.start()
    for delta in DELTAS:
        for k in range(3):
            if delta != 2:
                first(k, delta).start()
            first_info(k, delta).start()
    for k in range(3):
        for copy in keep(k):
            copy.wait()
        second_all(k, 0)
    for j in DELTAS:
        for k in range(3):
            if j == 2:
                for way in range(2):
                    piece = t2.at[(*at(k, 2, 0), pl.ds(rows // 2 * way, rows // 2), cols(k))]
                    remote(piece, piece, relay_s.at[k, way], relay_r.at[k, way], core, e).wait_recv()
            else:
                remote(block(k, j, 0), block(k, j, 0), s1s.at[k, 3 - j], s1r.at[k, 3 - j], core, e).wait_recv()
                relay(k, (3 - j) // 2).start()
            remote(info(k, j, 0), info(k, j, 0), m1s.at[k, 3 - j], m1r.at[k, 3 - j], core, e).wait_recv()
            second_all(k, j)

    @pl.loop(0, RING)
    def _(t):
        j = gray(t)
        for k in range(3):
            for way in range(2):
                came = block(k, j, 3 - 2 * way)
                remote(came, came, s2s.at[k, j, way], s2r.at[k, j, way], core, e).wait_recv()
                third(k, j, way).start()
            for delta in (1, 3):
                came = info(k, j, 4 - delta)
                remote(came, came, m2s.at[k, j, delta - 1], m2r.at[k, j, delta - 1], core, e).wait_recv()

        @pl.loop(0, 3)
        def _(d):
            for k in range(3):
                pick(k, t * 3 + d, j, d + d // 2)

    for k in range(3):
        for n in range(2):
            put(k, n, 0, 0).wait()

    def span(q):
        return pl.ds(half_slots * q, half_slots)

    def cube(q, o, k, p):
        return r.at[(q, o, *cube_at(k, p), slice(None), cols(k))]

    def rod(q, o, k, p, d1):
        at = list(cube_at(k, p))
        at[dims(k)[1]] = d1
        return r.at[(q, o, *at, slice(None), cols(k))]

    def rod_out(q, k, p, d1, to):
        at = (d1, slice(None)) if k == 2 else (slice(None), d1)
        return s_ref.at[(p, to, *at, span(q), cols(k))]

    def early(k, j1, delta, to):
        i1, i2 = dims(k)[1:]
        d1 = lax.rem(v[i1] + j1, RING)
        return remote(rod_out(0, k, lax.rem(v[i2] + delta, RING), d1, to), rod(0, core, k, v[i2], d1), xes.at[k, j1, delta, to], xer.at[k, j1, delta, core], to, step(e, v[i2], st[i2], delta))

    def late(k, delta, to):
        i2 = dims(k)[2]
        return remote(s_ref.at[lax.rem(v[i2] + delta, RING), to, :, :, span(1), cols(k)], cube(1, core, k, v[i2]), xs.at[1, k, delta, to], xr.at[1, k, delta, core], to, step(e, v[i2], st[i2], delta))

    def beside(q, k):
        i2 = dims(k)[2]
        return remote(s_ref.at[v[i2], 1 - core, :, :, span(q), cols(k)], cube(q, core, k, v[i2]), xs.at[q, k, 0, 0], xr.at[q, k, 0, 0], 1 - core, e)

    def inward(q, k):
        i2 = dims(k)[2]
        return pltpu.make_async_copy(s_ref.at[v[i2], core, :, :, span(q), cols(k)], cube(q, core, k, v[i2]), loc.at[0, q, k])


    @pl.loop(0, 3)
    def _(d):
        for delta in DELTAS:
            for k in range(3):
                for to in range(2):
                    early(k, d + d // 2, delta, to).start()

    for load in loads:
        load.start()

    @pl.loop(0, RING)
    def _(t):
        j = gray(t)
        for k in range(3):
            for way in range(2):
                came = t2.at[(*at(k, j, 2), pl.ds(rows // 2 * way, rows // 2), cols(k))]
                remote(came, came, s3s.at[k, j, way], s3r.at[k, j, way], core, e).wait_recv()
            came = info(k, j, 2)
            remote(came, came, m2s.at[k, j, 1], m2r.at[k, j, 1], core, e).wait_recv()
            pick(k, t, j, 2)

    for k in range(3):
        for n in range(2):
            put(k, n, 0, 0).wait()
    for delta in DELTAS:
        for k in range(3):
            for to in range(2):
                early(k, 2, delta, to).start()
    for q in range(2):
        for k in range(3):
            beside(q, k).start()
            inward(q, k).start()
    for delta in DELTAS:
        for k in range(3):
            for to in range(2):
                late(k, delta, to).start()
    for load in loads:
        load.wait()

    def z4_at(q, k, p, c):
        return z4.at[q, p, c, :, :, :, cols(k)]

    def back(q, o, k, delta):
        i2 = dims(k)[2]
        here = views[o][i2]
        return remote(cube(q, o, k, lax.rem(here + delta, RING)), z4_at(q, k, here, core), s4.at[q, k, delta, o], r4.at[q, k, delta, core], o, step(e, here, STRIDES[o][i2], delta))

    def across(q, k):
        i2 = dims(k)[2]
        return remote(cube(q, 1 - core, k, other[i2]), z4_at(q, k, other[i2], core), s4.at[q, k, 0, 0], r4.at[q, k, 0, 0], 1 - core, e)

    def stay(q, k):
        i2 = dims(k)[2]
        return pltpu.make_async_copy(cube(q, core, k, v[i2]), z4_at(q, k, v[i2], core), loc.at[1, q, k])

    @pl.loop(0, 2)
    def _(q):
        for k in range(3):
            i1, i2 = dims(k)[1:]
            inward(q, k).wait()
            target = cube(q, 1 - core, k, other[i2])
            remote(target, target, xs.at[q, k, 0, 0], xr.at[q, k, 0, 0], core, e).wait_recv()

        @pl.when(q == 0)
        def _():
            @pl.loop(0, RING)
            def _(j1):
                for k in range(3):
                    i1, i2 = dims(k)[1:]
                    for delta in DELTAS:
                        for o in range(2):
                            target = rod(0, o, k, lax.rem(views[o][i2] + 4 - delta, RING), lax.rem(views[o][i1] + j1, RING))
                            remote(target, target, xes.at[k, j1, delta, 0], xer.at[k, j1, delta, o], core, e).wait_recv()

        @pl.when(q == 1)
        def _():
            for k in range(3):
                i2 = dims(k)[2]
                for delta in DELTAS:
                    for o in range(2):
                        target = cube(1, o, k, lax.rem(views[o][i2] + 4 - delta, RING))
                        remote(target, target, xs.at[1, k, delta, 0], xr.at[1, k, delta, o], core, e).wait_recv()

        for o in range(2):
            @pl.loop(0, RING)
            def _(i):
                x = r[q, o, i].reshape(RING * RING * half_slots, r.shape[-1])
                gate = jnp.dot(x, wg[...], preferred_element_type=jnp.float32)
                up = jnp.dot(x, wu[...], preferred_element_type=jnp.float32)
                hidden = (jax.nn.silu(gate) * up).astype(jnp.bfloat16)
                y = jnp.dot(hidden, wd[...], preferred_element_type=jnp.float32).astype(jnp.bfloat16)
                r[q, o, i] = y.reshape(RING, RING, half_slots, r.shape[-1])

            for delta in DELTAS:
                for k in range(3):
                    back(q, o, k, delta).start()
        for k in range(3):
            across(q, k).start()
            stay(q, k).start()

    def line(q, k, p):
        at = (slice(None), slice(None), p, slice(None)) if k == 2 else (slice(None), slice(None), slice(None), p)
        return z4.at[(q, *at, slice(None), cols(k))]

    def forth(q, k, delta):
        i1 = dims(k)[1]
        return remote(line(q, k, lax.rem(v[i1] + delta, RING)), z5.at[v[i1], :, :, :, span(q), cols(k)], s5.at[q, k, delta - 1], r5.at[q, k, delta - 1], core, step(e, v[i1], st[i1], delta))

    def turn_delta(turn):
        h = turn // 2
        return (1 - h) * (2 - turn) + h * (9 - 3 * turn)

    def column(turn, k, from_d1):
        d0 = lax.rem(v[dims(k)[0]] + turn_delta(turn), RING)
        return z5.at[from_d1, :, :, d0, span(1), cols(k)]

    def single(turn, k, delta):
        i0, i1, _ = dims(k)
        d0, d1 = lax.rem(v[i0] + turn_delta(turn), RING), lax.rem(v[i1] + delta, RING)
        src = z4.at[(1, slice(None), slice(None), *plane_at(k, d0, d1), slice(None), cols(k))]
        return remote(src, column(turn, k, v[i1]), s6.at[k, turn, delta - 1], r6.at[k, turn, delta - 1], core, step(e, v[i1], st[i1], delta))

    def lift(q, k, stage):
        i1 = dims(k)[1]
        room = bounce.at[q, :, :, :, :, cols(k)]
        if stage == 0:
            return pltpu.make_async_copy(line(q, k, v[i1]), room, loc.at[2, q, k])
        return pltpu.make_async_copy(room, z5.at[v[i1], :, :, :, span(q), cols(k)], loc.at[3, q, k])

    for q in range(2):
        for k in range(3):
            i2 = dims(k)[2]
            stay(q, k).wait()
            target = z4_at(q, k, v[i2], 1 - core)
            remote(target, target, s4.at[q, k, 0, 0], r4.at[q, k, 0, 0], core, e).wait_recv()
            for delta in DELTAS:
                for o in range(2):
                    target = z4_at(q, k, lax.rem(v[i2] + 4 - delta, RING), o)
                    remote(target, target, s4.at[q, k, delta, 0], r4.at[q, k, delta, o], core, e).wait_recv()
            if q == 0:
                for delta in DELTAS:
                    forth(q, k, delta).start()
            lift(q, k, 0).start()
        if q == 1:
            @pl.loop(0, RING)
            def _(turn):
                for k in range(3):
                    for delta in DELTAS:
                        single(turn, k, delta).start()

        for k in range(3):
            lift(q, k, 0).wait()
            lift(q, k, 1).start()
    @pl.loop(0, RING)
    def _(j):
        for k in range(3):
            for way in range(2):
                second(k, j, way).wait_send()
                third(k, j, way).wait_send()

    for k in range(3):
        for way in range(2):
            relay(k, way).wait_send()

    @pl.loop(0, 2)
    def _(q):
        for k in range(3):
            across(q, k).wait_send()
            for delta in DELTAS:
                for o in range(2):
                    back(q, o, k, delta).wait_send()

    def fetch(q, turn, k, c):
        d0 = lax.rem(v[dims(k)[0]] + turn_delta(turn), RING)
        return pltpu.make_async_copy(z5.at[:, :, c, d0, span(q), cols(k)], t2.at[:, :, pl.ds(32 * (RING * q + turn) + half_slots * c, half_slots), cols(k)], load_sem.at[q, turn, k, c])

    def near(k, delta, part):
        i0 = dims(k)[0]
        at = pl.ds(rows // 2 * part, rows // 2)
        way = delta // 2
        return remote(sums.at[delta, at, cols(k)], came2.at[way, at, cols(k)], ps.at[k, way, part], pr.at[k, way, part], core, step(e, v[i0], st[i0], delta))

    def far(k, way):
        i0 = dims(k)[0]
        at = pl.ds(rows // 2 * way, rows // 2)
        return remote(sums.at[2, at, cols(k)], passing.at[way, :, cols(k)], hs.at[k, way], hr.at[k, way], core, step(e, v[i0], st[i0], 1 + 2 * way))

    def join(k, delta):
        way = delta // 2
        at = pl.ds(rows // 2 * way, rows // 2)
        remote(passing.at[way, :, cols(k)], passing.at[way, :, cols(k)], hs.at[k, way], hr.at[k, way], core, e).wait_recv()
        sums[delta, at, cols(k)] += passing[way, :, cols(k)]
        near(k, delta, way).start()

    n = RING * RING * 2 * half_slots
    lane = lax.broadcasted_iota(jnp.int32, (1, n), 1)
    place_of = (lane // (RING * 2 * half_slots), (lane // (2 * half_slots)) % RING, (lane // half_slots) % 2, lane % half_slots)

    def weights(q, delta, k):
        d1, p2, half, s = place_of
        i0, i1, i2 = dims(k)
        a, b = at(k, delta, 0)
        m = jnp.transpose(mt[k, a, b])
        key = ((half * 64 + v[i0] * st[i0] + d1 * st[i1] + p2 * st[i2]) * slots + half_slots * q + s).astype(jnp.float32)
        w = jnp.zeros((rows, n), jnp.float32)
        for j in range(8):
            w = jnp.where(m[:, j:j + 1] == key, m[:, 8 + j:9 + j], w)
        hi = w.astype(jnp.bfloat16)
        rest = w - hi.astype(jnp.float32)
        mid = rest.astype(jnp.bfloat16)
        low = (rest - mid.astype(jnp.float32)).astype(jnp.bfloat16)
        return low, mid, hi

    def weigh(q, turn, k, terms):
        for c in range(2):
            fetch(q, turn, k, c).wait()
        y = t2[:, :, pl.ds(32 * (RING * q + turn), 32), cols(k)].reshape(n, COLS[k][1])
        got = jnp.dot(jnp.concatenate(terms, axis=0), y, preferred_element_type=jnp.float32)
        return (got[:rows] + got[rows:2 * rows]) + got[2 * rows:]

    @pl.loop(0, RING)
    def _(turn):
        for k in range(3):
            for i, term in enumerate(weights(1, turn_delta(turn), k)):
                r[k // 2, k % 2, turn, :, :, :, pl.ds(n * i, n)] = term.reshape(RING, RING, half_slots, n)

    for q in range(2):
        for k in range(3):
            lift(q, k, 1).wait()
        if q == 0:
            for k in range(3):
                i1 = dims(k)[1]
                for delta in DELTAS:
                    target = z5.at[lax.rem(v[i1] + 4 - delta, RING), :, :, :, span(0), cols(k)]
                    remote(target, target, s5.at[0, k, delta - 1], r5.at[0, k, delta - 1], core, e).wait_recv()
                for turn in range(RING):
                    for c in range(2):
                        fetch(0, turn, k, c).start()

        @pl.loop(0, RING)
        def _(turn):
            delta = turn_delta(turn)
            if q == 1:
                for k in range(3):
                    i1 = dims(k)[1]
                    for d in DELTAS:
                        target = column(turn, k, lax.rem(v[i1] + 4 - d, RING))
                        remote(target, target, s6.at[k, turn, d - 1], r6.at[k, turn, d - 1], core, e).wait_recv()
                    for c in range(2):
                        fetch(1, turn, k, c).start()
            for k in range(3):
                if q == 0:
                    sums[delta, :, cols(k)] = weigh(q, turn, k, weights(q, delta, k))
                else:
                    terms = [r[k // 2, k % 2, turn, :, :, :, pl.ds(n * i, n)].reshape(rows, n) for i in range(3)]
                    sums[delta, :, cols(k)] += weigh(q, turn, k, terms)

                    @pl.when(turn == 0)
                    def _():
                        for way in range(2):
                            far(k, way).start()

                    @pl.when(turn == 1)
                    def _():
                        near(k, 1, 1).start()

                    @pl.when(turn == 2)
                    def _():
                        near(k, 3, 0).start()

    for k in range(3):
        join(k, 1)
    for k in range(3):
        join(k, 3)
    keep = pltpu.make_async_copy(sums.at[0], own, load_sem.at[0, 0, 0, 0])
    keep.start()
    for k in range(3):
        for way in range(2):
            for part in range(2):
                target = came2.at[way, pl.ds(rows // 2 * part, rows // 2), cols(k)]
                remote(target, target, ps.at[k, way, part], pr.at[k, way, part], core, e).wait_recv()
    keep.wait()

    @pl.loop(0, RING)
    def _(j):
        for k in range(3):
            for delta in DELTAS:
                single(j, k, delta).wait_send()
                second_info(k, j, delta).wait_send()
                for to in range(2):
                    early(k, j, delta, to).wait_send()

    for k in range(3):
        for delta in DELTAS:
            if delta != 2:
                first(k, delta).wait_send()
            first_info(k, delta).wait_send()
            forth(0, k, delta).wait_send()
            for to in range(2):
                late(k, delta, to).wait_send()

    for k in range(3):
        for way in range(2):
            far(k, way).wait_send()
            for part in range(2):
                near(k, 1 + 2 * way, part).wait_send()

    @pl.loop(0, 2)
    def _(q):
        for k in range(3):
            beside(q, k).wait_send()


def solution(mesh):
    group_axes = ("node", "expert")
    group_size = mesh.shape["node"] * mesh.shape["expert"]
    tok_spec = P(("data", "node", "expert"), None)
    weight_spec = P(("node", "expert"), None, None)
    hbm = pl.BlockSpec(memory_space=pltpu.HBM)
    vmem = pl.BlockSpec(memory_space=pltpu.VMEM)
    dma = pltpu.SemaphoreType.DMA

    def local_layer(tokens, expert_ids, gate_weights, slot_ids, w_gate, w_up, w_down):
        rows, width = tokens.shape
        top_k = expert_ids.shape[1]
        slots = capacity(rows, top_k, group_size)
        bf = jnp.bfloat16
        f32 = jnp.float32
        own, came = pl.pallas_call(
            lambda *refs: layer_kernel(slots, *refs),
            name="layer",
            in_specs=[vmem] * 4 + [hbm] * 3,
            out_specs=[hbm] * 5,
            out_shape=[
                jax.ShapeDtypeStruct((4, 2, 4, 4, slots, width), bf), jax.ShapeDtypeStruct((2, 4, 2, 4, 4, slots // 2, width), bf),
                jax.ShapeDtypeStruct((4, 4, 2, 4, slots, width), bf), jax.ShapeDtypeStruct((rows, width), f32), jax.ShapeDtypeStruct((2, rows, width), f32),
            ],
            scratch_shapes=[pltpu.VMEM((3, 4, 4, 16, rows), f32), pltpu.VMEM((4, 4, rows, width), bf)] + [pltpu.VMEM((2, 4, 2, slots, n), bf) for _, n in COLS]
            + [pltpu.VMEM((2, 2, 4, 4, 4, slots // 2, width), bf), pltpu.VMEM((2, 4, 2, 4, slots // 2, width), bf)]
            + [pltpu.VMEM(w.shape[1:], bf) for w in (w_gate, w_up, w_down)]
            + [pltpu.VMEM((4, rows, width), f32), pltpu.VMEM((2, rows // 2, width), f32)]
            + [dma((2, 3)), dma((3, 2))] + [dma((3, 3))] * 4 + [dma((3, 4, 2))] * 2 + [dma((3, 4, 3))] * 2 + [dma((3, 4, 2))] * 2
            + [dma((3,)), dma((4, 2, 3))] + [dma((3, 4, 4, 2))] * 2 + [dma((2, 3, 4, 2))] * 4 + [dma((2, 3, 3))] * 2
            + [dma((3, 2))] * 2 + [dma((2, 4, 3, 2))] + [dma((3, 2))] * 2 + [dma((3, 2, 2))] * 2
            + [dma((3, 4, 3))] * 2 + [pltpu.VMEM((16, rows), f32)],
            compiler_params=pltpu.CompilerParams(collective_id=1, has_side_effects=True, vmem_limit_bytes=67043328),
        )(tokens, expert_ids.T, slot_ids.T, gate_weights.T, w_gate, w_up, w_down)[3:]
        return (own + (came[0] + came[1])).astype(bf)

    return jax.shard_map(local_layer, mesh=mesh, in_specs=(tok_spec, tok_spec, tok_spec, tok_spec, weight_spec, weight_spec, weight_spec), out_specs=tok_spec, check_vma=False)
```
